32 devices in a mesh: slab: 16 (over z, y, x), comp: 2 (over core).
Axes of the slice: x: 2, y: 2, z: 4, core: 2. Of those that a mesh axis runs over, the one named last changes fastest.
Arguments:
- polarization: float32 [6, 16, 128, 128], P('comp', 'slab'), parts along dimension 0, may hold values from -6 to 6
- inverse_polarizability: float32 [16, 128, 128], P('slab'), may hold values from 0.5 to 2
- occupancy: int32 [16, 16, 16], P('slab'), may hold values 0 or 1
- green_fourier: float32 [6, 256, 32, 256], P(None, 'slab'), may hold values from -12 to 12
Outputs:
- first_image: float32 [6, 16, 128, 128], P('comp', 'slab'), parts along dimension 0
- second_image: float32 [6, 16, 128, 128], P('comp', 'slab'), parts along dimension 0
The draws below stay inside these ranges and needn't reach their ends.
There are 2 independent parts, one for each index of `comp`. The reference program is written for one: setup_inputs(seed, part) draws one part's arguments, and reference() takes and returns one part's arrays. A program takes and returns all parts, laid end to end along the dimension named above; an argument that names none is the same for every part. Nothing has to cross between parts.
All inputs are finite; a program needn't handle non-finite values. No bound on the sum of `occupancy` on one device may be relied on, other than what follows from the above.
Results may differ from the reference program's by a relative error of at most 0.0001.
Values sent between devices are 32-bit elements; how exact they have to be, the bound alone decides.
A program may use at most 64 MiB of HBM per device.

```python
import math
import jax
import jax.numpy as jnp

NY = 128
NZ = 128
BLOCK = 8
MATVECS = 2
NX = 16
LX = 32
LY = 256
LZ = 256


def plant(entries, own_key, smallest, largest):
    index_at = [jax.random.randint(jax.random.fold_in(own_key, axis), (), 0, length) for axis, length in enumerate(entries.shape)]
    main_axis = entries.shape.index(max(entries.shape))
    beside = index_at[:main_axis] + [(index_at[main_axis] + 1) % entries.shape[main_axis]] + index_at[main_axis + 1:]
    return entries.at[tuple(index_at)].set(smallest).at[tuple(beside)].set(largest)


def block_scale(own_key, dims, pieces, least, top_value):
    gain, own = 1.0, jax.random.fold_in(own_key, 6)
    for position, shards_of in pieces:
        heights = jnp.exp(jax.random.uniform(jax.random.fold_in(own, position), (shards_of,), jnp.float32, least / len(pieces), top_value / len(pieces)))
        gain = gain * jnp.repeat(heights, dims[position] // shards_of).reshape([-1 if axis == position else 1 for axis in range(len(dims))])
    return gain


def centred(key, extent, width, reach, shards=(), dtype=jnp.bfloat16):
    factor_of = block_scale(key, extent, shards, -0.22, 0.18) if shards else 1.0
    result = jax.random.normal(key, extent, jnp.float32) * width * factor_of
    return jnp.minimum(jnp.maximum(result, -reach), reach).astype(dtype)


def setup_inputs(seed: int = 0, part: int = 0) -> dict:
    arg_keys = jax.random.split(jax.random.key(seed), 5)
    part_splits = jax.random.split(jax.random.fold_in(arg_keys[4], part), 5)
    polarization = centred(part_splits[0], (3, NX, NY, NZ), 1.0, 6.0, ((1, 16),), jnp.float32)
    inverse_polarizability = jnp.clip(jnp.exp(math.log(2.0) - 1.3862944 * jax.random.uniform(arg_keys[1], (NX, NY, NZ), jnp.float32) ** block_scale(arg_keys[1], (NX, NY, NZ), ((0, 16),), -0.2, 0.2)), 0.5, 2.0)
    occupancy = plant((jax.random.randint(arg_keys[2], (NX, NY // BLOCK, NZ // BLOCK), 0, 4) < 3).astype(jnp.int32), jax.random.fold_in(arg_keys[2], 1), 0, 1)
    green_fourier = centred(arg_keys[3], (6, LZ, LX, LY), 2.0, 12.0, ((1, 16),), jnp.float32)
    return dict(polarization=polarization, inverse_polarizability=inverse_polarizability, occupancy=occupancy, green_fourier=green_fourier)


def expand_mask(occupancy):
    flags = occupancy.astype(jnp.float32)
    first, second, third = flags.shape
    spread = jnp.broadcast_to(flags[:, :, None, :, None], (first, second, BLOCK, third, BLOCK))
    return spread.reshape(first, second * BLOCK, third * BLOCK)


def apply_operator(field, mask, inverse_polarizability, green_ordered):
    masked = field * mask[None]
    padded = jnp.pad(masked, ((0, 0), (0, NX), (0, NY), (0, NZ)))
    spectrum = jnp.fft.fftn(padded, axes=(1, 2, 3))
    combos = ((0, 3, 4), (3, 1, 5), (4, 5, 2))
    results = []
    for row in combos:
        product = green_ordered[row[0]] * spectrum[0] + green_ordered[row[1]] * spectrum[1] + green_ordered[row[2]] * spectrum[2]
        back = jnp.fft.ifftn(product).real[:NX, :NY, :NZ]
        results.append(back.astype(jnp.float32))
    convolved = jnp.stack(results)
    return inverse_polarizability[None] * masked - mask[None] * convolved


def reference(polarization, inverse_polarizability, occupancy, green_fourier):
    mask = expand_mask(occupancy)
    green_ordered = jnp.transpose(green_fourier, (0, 2, 3, 1))
    first_image = apply_operator(polarization, mask, inverse_polarizability, green_ordered)
    current = first_image
    for repeat_index in range(MATVECS - 1):
        current = apply_operator(current, mask, inverse_polarizability, green_ordered)
    return first_image, current
```

```python
import functools
import math

import jax
import jax.numpy as jnp
import numpy as np
from jax import lax
from jax.experimental import pallas as pl
from jax.experimental.pallas import tpu as pltpu
from jax.sharding import PartitionSpec as P

BLOCK = 8
MATVECS = 2
F32 = jnp.float32
BF16 = jnp.bfloat16
COMBOS = ((0, 3, 4), (3, 1, 5), (4, 5, 2))


def tables(count_in, count_out, length):
    phase = np.arange(count_in)[:, None] * np.arange(count_out)[None, :] % length
    angle = phase * (2.0 * math.pi / length)
    return np.cos(angle), np.sin(angle)


def split_table(table):
    table = table.astype(np.float32)
    high = table.astype(jnp.bfloat16)
    low = (table - high.astype(np.float32)).astype(jnp.bfloat16)
    return high, low


def split(value):
    high = value.astype(BF16)
    return high, (value - high.astype(F32)).astype(BF16)


def twiddle(re, im, num, length, sign):
    num = num * sign % length
    if num == 0:
        return re, im
    if 4 * num == length:
        return -im, re
    if 2 * num == length:
        return -re, -im
    if 4 * num == 3 * length:
        return im, -re
    c = math.cos(2.0 * math.pi * num / length)
    s = math.sin(2.0 * math.pi * num / length)
    if (8 * num) % length == 0:
        a = abs(c)
        p, m = (re + im) * a, (re - im) * a
        return {1: (m, p), 3: (-p, m), 5: (-m, -p), 7: (p, -m)}[8 * num // length]
    return re * c - im * s, re * s + im * c


def fft(values, sign):
    n = len(values)
    if n == 1:
        return values
    even, odd = fft(values[0::2], sign), fft(values[1::2], sign)
    low, high = [], []
    for k in range(n // 2):
        (er, ei), (o_r, oi) = even[k], twiddle(*odd[k], k, n, sign)
        low.append((er + o_r, ei + oi))
        high.append((er - o_r, ei - oi))
    return low + high


def three_pass(pair, table_pair, dims):
    dot = functools.partial(lax.dot_general, dimension_numbers=dims, preferred_element_type=F32)
    (vh, vl), (th, tl) = pair, table_pair
    return dot(vh, th) + (dot(vl, th) + dot(vh, tl))


def kernel(
    n, cells_x, padded_x, kz_own, kc,
    pol_hbm, inv_hbm, occ_hbm, green_ref, *refs,
):
    tables_hbm, refs = refs[:8], refs[8:]
    first_ref, second_ref, pol_ref, inv_ref, occ_ref, *refs = refs
    tables_vmem, refs = refs[:8], refs[8:]
    wz_h, wz_l, wy_h, wy_l, vy_h, vy_l, vz_h, vz_l = tables_vmem
    (
        green_raw, green, mask_ref, raw_out, raw_in, out_t, in_t, lines, spec, out_u, in_u, part_out, part_in,
        green_sem, load_sem, ws_sem, wr_sem, ts_sem, tr_sem, cs_sem, cr_sem, os_sem, or_sem, ps_sem, pr_sem,
    ) = refs
    me = lax.axis_index("slab")
    group = n // 2
    here = me // group
    seat = lax.rem(me, group)
    twin = lax.rem(me + group, n)
    base = here * group
    chunks = kz_own // kc
    cells_y, cells_z = mask_ref.shape
    padded_y = 2 * cells_y
    halves = padded_y // 128

    def signal(device):
        pl.semaphore_signal(barrier, inc=1, device_id={"slab": device}, device_id_type=pl.DeviceIdType.MESH)

    def remote(source, target, send_sem, recv_sem, device):
        return pltpu.make_async_remote_copy(
            src_ref=source, dst_ref=target, send_sem=send_sem, recv_sem=recv_sem,
            device_id={"slab": device}, device_id_type=pl.DeviceIdType.MESH,
        )

    barrier = pltpu.get_barrier_semaphore()
    signal(twin)

    def greet(k, carry):
        signal(base + lax.rem(seat + k, group))
        return carry

    lax.fori_loop(1, group, greet, 0)
    sources = (occ_hbm, pol_hbm, inv_hbm, *tables_hbm)
    targets = (occ_ref, pol_ref, inv_ref, *tables_vmem)
    loads = [
        pltpu.make_async_copy(source, target, load_sem.at[i]) for i, (source, target) in enumerate(zip(sources, targets))
    ]
    for load in loads:
        load.start()
    green_copy = pltpu.make_async_copy(green_ref, green_raw, green_sem)
    green_copy.start()
    loads[0].wait()

    blocks_y, blocks_z = occ_ref.shape[1:]
    up_y = lax.broadcasted_iota(jnp.int32, (cells_y, blocks_y), 0) // BLOCK
    up_y = (up_y == lax.broadcasted_iota(jnp.int32, (cells_y, blocks_y), 1)).astype(F32).astype(BF16)
    up_z = lax.broadcasted_iota(jnp.int32, (blocks_z, cells_z), 1) // BLOCK
    up_z = (up_z == lax.broadcasted_iota(jnp.int32, (blocks_z, cells_z), 0)).astype(F32).astype(BF16)
    flags = occ_ref[0].astype(F32).astype(BF16)
    spread = jnp.dot(up_y, flags, preferred_element_type=F32).astype(BF16)
    mask_ref[...] = jnp.dot(spread, up_z, preferred_element_type=F32)

    def order_green():
        green_copy.wait()

        def one(g, carry):
            for j in range(chunks):
                for t in range(0, padded_x, 8):
                    tile = green_raw[g, j * kc:(j + 1) * kc, t:t + 8, :]
                    tile = jnp.swapaxes(tile, 0, 1)
                    for h in range(halves):
                        green[j * halves + h, g, t:t + 8] = tile[:, :, h * 128:(h + 1) * 128]
            return carry

        lax.fori_loop(0, 6, one, 0)

    def send_raw(step, c, field):
        raw_out[c] = field
        remote(raw_out.at[c], raw_in.at[c], ws_sem.at[step, c], wr_sem.at[step, c], twin).start()

    def forward_z(c, which, field):
        dims = (((1,), (1,)), ((), ()))
        res = three_pass((wz_h[here], wz_l[here]), split(field), dims)
        out_t[c, which] = res.reshape(chunks, group, 2, kc, cells_y)

    def send_block(step, c, which, j):
        slab = me if which == 0 else twin

        def send(k, carry):
            to = lax.rem(seat + k, group)
            remote(
                out_t.at[c, which, j, to], in_t.at[c, j, slab], ts_sem.at[step, c, j], tr_sem.at[step, c, j], base + to
            ).start()
            return carry

        lax.fori_loop(1, group, send, 0)
        in_t[c, j, slab] = out_t[c, which, j, seat]

    def drain(view, sem):
        pltpu.make_async_copy(view, view, sem).wait()

    def forward_yx(step, c, j):
        drain(in_t.at[c, j, pl.ds(0, n - 2)], tr_sem.at[step, c, j])
        parts = [in_t[c, j, :, part].reshape(cells_x * kc, cells_y) for part in range(2)]
        dims = (((1,), (0,)), ((), ()))
        res = three_pass(split(jnp.concatenate(parts, axis=1)), (wy_h[...], wy_l[...]), dims)
        for part in range(2):
            for h in range(halves):
                at = part * padded_y + h * 128
                lines[j * halves + h, part] = res[:, at:at + 128].reshape(cells_x, kc, 128)

        def columns(h, carry):
            i = j * halves + h
            line = [(lines[i, 0, x], lines[i, 1, x]) for x in range(cells_x)]
            for m, (re, im) in enumerate(fft(line, -1)):
                spec[i, 2 * c, 2 * m], spec[i, 2 * c + 1, 2 * m] = re, im
            line = [twiddle(lines[i, 0, x], lines[i, 1, x], x, padded_x, -1) for x in range(cells_x)]
            for m, (re, im) in enumerate(fft(line, -1)):
                spec[i, 2 * c, 2 * m + 1], spec[i, 2 * c + 1, 2 * m + 1] = re, im
            return carry

        lax.fori_loop(0, halves, columns, 0)

    def backward_xy(step, a, j):
        row = COMBOS[a]

        def columns(h, carry):
            i = j * halves + h

            def field(k):
                g = [green[i, r, k] for r in row]
                s = [spec[i, r, k] for r in range(6)]
                return g[0] * s[0] + g[1] * s[2] + g[2] * s[4], g[0] * s[1] + g[1] * s[3] + g[2] * s[5]

            even = fft([field(k) for k in range(0, padded_x, 2)], 1)
            for x in range(cells_x):
                lines[i, 0, x], lines[i, 1, x] = even[x]
            odd = fft([field(k) for k in range(1, padded_x, 2)], 1)
            for x in range(cells_x):
                re, im = twiddle(*odd[x], x, padded_x, 1)
                lines[i, 0, x] += re
                lines[i, 1, x] += im
            return carry

        lax.fori_loop(0, halves, columns, 0)
        parts = [
            lines[j * halves + h, part].reshape(cells_x * kc, 128) for part in range(2) for h in range(halves)
        ]
        dims = (((1,), (0,)), ((), ()))
        res = three_pass(split(jnp.concatenate(parts, axis=1)), (vy_h[...], vy_l[...]), dims)
        for part in range(2):
            piece = res[:, part * cells_y:(part + 1) * cells_y]
            out_u[a, j, :, part] = piece.reshape(cells_x, kc, cells_y)
        send_back(step, a, j, 1, (1 - here) * group, cs_sem, cr_sem)
        send_back(step, a, j, 0, base, os_sem, or_sem)

    def send_back(step, a, j, which, first, s_sem, r_sem):
        def send(k, carry):
            to = lax.rem(seat + k, group)
            remote(
                out_u.at[a, j, first + to], in_u.at[a, which, j, seat], s_sem.at[step, a, j], r_sem.at[step, a, j],
                base + to,
            ).start()
            return carry

        lax.fori_loop(1, group, send, 0)
        in_u[a, which, j, seat] = out_u[a, j, first + seat]

    def inverse_z(a, which):
        field = in_u[a, which].reshape(chunks * group * 2 * kc, cells_y)
        return three_pass(split(field), (vz_h[here], vz_l[here]), (((0,), (0,)), ((), ())))

    def send_part(step, a):
        for j in range(chunks):
            drain(in_u.at[a, 1, j, pl.ds(0, group - 1)], cr_sem.at[step, a, j])
        part_out[a] = inverse_z(a, 1)
        remote(part_out.at[a], part_in.at[a], ps_sem.at[step, a], pr_sem.at[step, a], twin).start()

    loads[1].wait()
    for step in range(MATVECS):
        source, image = (pol_ref, first_ref) if step == 0 else (first_ref, second_ref)
        if step == 0:
            pl.semaphore_wait(barrier, group)
            for c in range(3):
                send_raw(step, c, source[c, 0] * mask_ref[...])
            for load in loads[2:]:
                load.wait()
            for c in range(3):
                forward_z(c, 0, raw_out[c])
                send_block(step, c, 0, 0)
            for j in range(1, chunks):
                for c in range(3):
                    send_block(step, c, 0, j)
            order_green()
        for c in range(3):
            drain(raw_in.at[c], wr_sem.at[step, c])
            forward_z(c, 1, raw_in[c])
            send_block(step, c, 1, 0)
        for j in range(1, chunks):
            for c in range(3):
                send_block(step, c, 1, j)
        for j in range(chunks):
            for c in range(3):
                forward_yx(step, c, j)
            for a in range(3):
                backward_xy(step, a, j)
                if j == chunks - 1 and a > 0:
                    send_part(step, a - 1)
        send_part(step, 2)
        for c in range(3):
            drain(raw_out.at[c], ws_sem.at[step, c])
            for j in range(chunks):
                drain(in_t.at[c, j, pl.ds(0, n - 2)], ts_sem.at[step, c, j])
        for a in range(3):
            for j in range(chunks):
                drain(in_u.at[a, 0, j, pl.ds(0, group - 1)], or_sem.at[step, a, j])
            own = inverse_z(a, 0)
            masked = source[a, 0] * mask_ref[...]
            drain(part_in.at[a], pr_sem.at[step, a])
            image[a, 0] = inv_ref[0] * masked - mask_ref[...] * (own + part_in[a])
            if step + 1 < MATVECS:
                send_raw(step + 1, a, image[a, 0] * mask_ref[...])
                forward_z(a, 0, raw_out[a])
                for j in range(chunks):
                    send_block(step + 1, a, 0, j)
        for a in range(3):
            for j in range(chunks):
                drain(in_u.at[a, 1, j, pl.ds(0, group - 1)], cs_sem.at[step, a, j])
                drain(in_u.at[a, 0, j, pl.ds(0, group - 1)], os_sem.at[step, a, j])
            drain(part_out.at[a], ps_sem.at[step, a])


def deliver(first_ref, second_ref, first_out, second_out, first, second, in_sem, out_sem):
    loads = [
        pltpu.make_async_copy(source, held, in_sem.at[i])
        for i, (source, held) in enumerate(((first_ref, first), (second_ref, second)))
    ]
    stores = [
        pltpu.make_async_copy(held, target, out_sem.at[i])
        for i, (held, target) in enumerate(((first, first_out), (second, second_out)))
    ]
    for copy in loads:
        copy.start()
    for load, store in zip(loads, stores):
        load.wait()
        store.start()
    for store in stores:
        store.wait()


def per_device(n, polarization, inverse_polarizability, occupancy, green_fourier):
    _, _, cells_y, cells_z = polarization.shape
    _, kz_own, padded_x, padded_y = green_fourier.shape
    padded_z = 2 * cells_z
    cells_x = padded_x // 2
    kc = min(8, kz_own)
    chunks = kz_own // kc
    halves = padded_y // 128
    group = n // 2

    def by_block(table):
        table = table.reshape(2, 2, group, chunks, kc, cells_z)
        return table.transpose(1, 3, 2, 0, 4, 5).reshape(2, chunks * group * 2 * kc, cells_z)

    cos, sin = tables(padded_z, cells_z, padded_z)
    wz = split_table(by_block(np.stack([cos, -sin])))
    vz = split_table(by_block(np.stack([cos, -sin])) / (padded_x * padded_y * padded_z))
    cos, sin = tables(cells_y, padded_y, padded_y)
    wy = split_table(np.block([[cos, -sin], [sin, cos]]))
    cos, sin = tables(padded_y, cells_y, padded_y)
    vy = split_table(np.block([[cos, sin], [-sin, cos]]))
    constants = [jnp.asarray(table) for table in wz + wy + vy + vz]
    anywhere = pl.BlockSpec(memory_space=pl.ANY)
    vmem = pl.BlockSpec(memory_space=pltpu.VMEM)
    dma = pltpu.SemaphoreType.DMA
    images = pl.pallas_call(
        functools.partial(kernel, n, cells_x, padded_x, kz_own, kc),
        out_shape=(jax.ShapeDtypeStruct(polarization.shape, F32),) * 2,
        in_specs=[anywhere] * 12,
        out_specs=(vmem, vmem),
        scratch_shapes=[
            pltpu.VMEM(polarization.shape, F32),
            pltpu.VMEM(inverse_polarizability.shape, F32),
            pltpu.VMEM(occupancy.shape, jnp.int32),
            *[pltpu.VMEM(table.shape, BF16) for table in constants],
            pltpu.VMEM(green_fourier.shape, F32),
            pltpu.VMEM((chunks * halves, 6, padded_x, kc, 128), F32),
            pltpu.VMEM((cells_y, cells_z), F32),
            pltpu.VMEM((3, cells_y, cells_z), F32),
            pltpu.VMEM((3, cells_y, cells_z), F32),
            pltpu.VMEM((3, 2, chunks, group, 2, kc, cells_y), F32),
            pltpu.VMEM((3, chunks, n, 2, kc, cells_y), F32),
            pltpu.VMEM((chunks * halves, 2, cells_x, kc, 128), F32),
            pltpu.VMEM((chunks * halves, 6, padded_x, kc, 128), F32),
            pltpu.VMEM((3, chunks, n, 2, kc, cells_y), F32),
            pltpu.VMEM((3, 2, chunks, group, 2, kc, cells_y), F32),
            pltpu.VMEM((3, cells_y, cells_z), F32),
            pltpu.VMEM((3, cells_y, cells_z), F32),
            dma,
            dma((11,)),
            *[dma((MATVECS, 3))] * 2,
            *[dma((MATVECS, 3, chunks))] * 6,
            *[dma((MATVECS, 3))] * 2,
        ],
        compiler_params=pltpu.CompilerParams(
            collective_id=0, has_side_effects=True, vmem_limit_bytes=60 * 1024 * 1024
        ),
    )(polarization, inverse_polarizability, occupancy, green_fourier, *constants)
    return pl.pallas_call(
        deliver,
        out_shape=(jax.ShapeDtypeStruct(polarization.shape, F32),) * 2,
        in_specs=[anywhere] * 2,
        out_specs=(anywhere, anywhere),
        scratch_shapes=[pltpu.VMEM(polarization.shape, F32)] * 2 + [pltpu.SemaphoreType.DMA((2,))] * 2,
    )(*images)


def solution(mesh):
    return jax.shard_map(
        functools.partial(per_device, mesh.shape["slab"]),
        mesh=mesh,
        in_specs=(
            P("comp", "slab", None, None),
            P("slab", None, None),
            P("slab", None, None),
            P(None, "slab", None, None),
        ),
        out_specs=(P("comp", "slab", None, None), P("comp", "slab", None, None)),
        check_vma=False,
    )
```

```python
import functools
import math

import jax
import jax.numpy as jnp
import numpy as np
from jax import lax
from jax.experimental import pallas as pl
from jax.experimental.pallas import tpu as pltpu
from jax.sharding import PartitionSpec as P

BLOCK = 8
MATVECS = 2
F32 = jnp.float32
BF16 = jnp.bfloat16
COMBOS = ((0, 3, 4), (3, 1, 5), (4, 5, 2))


def tables(count_in, count_out, length):
    phase = np.arange(count_in)[:, None] * np.arange(count_out)[None, :] % length
    angle = phase * (2.0 * math.pi / length)
    return np.cos(angle), np.sin(angle)


def split_table(table):
    table = table.astype(np.float32)
    high = table.astype(jnp.bfloat16)
    low = (table - high.astype(np.float32)).astype(jnp.bfloat16)
    return high, low


def split(value):
    high = value.astype(BF16)
    return high, (value - high.astype(F32)).astype(BF16)


def twiddle(re, im, num, length, sign):
    num = num * sign % length
    if num == 0:
        return re, im
    if 4 * num == length:
        return -im, re
    if 2 * num == length:
        return -re, -im
    if 4 * num == 3 * length:
        return im, -re
    c = math.cos(2.0 * math.pi * num / length)
    s = math.sin(2.0 * math.pi * num / length)
    if (8 * num) % length == 0:
        a = abs(c)
        p, m = (re + im) * a, (re - im) * a
        return {1: (m, p), 3: (-p, m), 5: (-m, -p), 7: (p, -m)}[8 * num // length]
    return re * c - im * s, re * s + im * c


def fft(values, sign):
    n = len(values)
    if n == 1:
        return values
    even, odd = fft(values[0::2], sign), fft(values[1::2], sign)
    low, high = [], []
    for k in range(n // 2):
        (er, ei), (o_r, oi) = even[k], twiddle(*odd[k], k, n, sign)
        low.append((er + o_r, ei + oi))
        high.append((er - o_r, ei - oi))
    return low + high


def three_pass(pair, table_pair, dims):
    dot = functools.partial(lax.dot_general, dimension_numbers=dims, preferred_element_type=F32)
    (vh, vl), (th, tl) = pair, table_pair
    return dot(vh, th) + (dot(vl, th) + dot(vh, tl))


def kernel(
    n, cells_x, padded_x, kz_own, kc,
    pol_hbm, inv_hbm, occ_hbm, green_ref, *refs,
):
    tables_hbm, refs = refs[:8], refs[8:]
    first_ref, second_ref, pol_ref, inv_ref, occ_ref, *refs = refs
    tables_vmem, refs = refs[:8], refs[8:]
    wz_h, wz_l, wy_h, wy_l, vy_h, vy_l, vz_h, vz_l = tables_vmem
    (
        green_raw, green, mask_ref, raw_out, raw_in, out_t, in_t, lines, spec, out_u, in_u, part_out, part_in,
        green_sem, load_sem, ws_sem, wr_sem, ts_sem, tr_sem, cs_sem, cr_sem, os_sem, or_sem, ps_sem, pr_sem,
    ) = refs
    me = lax.axis_index("slab")
    group = n // 2
    here = me // group
    seat = lax.rem(me, group)
    twin = lax.rem(me + group, n)
    base = here * group
    chunks = kz_own // kc
    cells_y, cells_z = mask_ref.shape
    padded_y = 2 * cells_y
    halves = padded_y // 128

    def signal(device):
        pl.semaphore_signal(barrier, inc=1, device_id={"slab": device}, device_id_type=pl.DeviceIdType.MESH)

    def remote(source, target, send_sem, recv_sem, device):
        return pltpu.make_async_remote_copy(
            src_ref=source, dst_ref=target, send_sem=send_sem, recv_sem=recv_sem,
            device_id={"slab": device}, device_id_type=pl.DeviceIdType.MESH,
        )

    barrier = pltpu.get_barrier_semaphore()
    signal(twin)

    def greet(k, carry):
        signal(base + lax.rem(seat + k, group))
        return carry

    lax.fori_loop(1, group, greet, 0)
    sources = (occ_hbm, pol_hbm, inv_hbm, *tables_hbm)
    targets = (occ_ref, pol_ref, inv_ref, *tables_vmem)
    loads = [
        pltpu.make_async_copy(source, target, load_sem.at[i]) for i, (source, target) in enumerate(zip(sources, targets))
    ]
    for load in loads:
        load.start()
    green_copy = pltpu.make_async_copy(green_ref, green_raw, green_sem)
    green_copy.start()
    loads[0].wait()

    blocks_y, blocks_z = occ_ref.shape[1:]
    up_y = lax.broadcasted_iota(jnp.int32, (cells_y, blocks_y), 0) // BLOCK
    up_y = (up_y == lax.broadcasted_iota(jnp.int32, (cells_y, blocks_y), 1)).astype(F32).astype(BF16)
    up_z = lax.broadcasted_iota(jnp.int32, (blocks_z, cells_z), 1) // BLOCK
    up_z = (up_z == lax.broadcasted_iota(jnp.int32, (blocks_z, cells_z), 0)).astype(F32).astype(BF16)
    flags = occ_ref[0].astype(F32).astype(BF16)
    spread = jnp.dot(up_y, flags, preferred_element_type=F32).astype(BF16)
    mask_ref[...] = jnp.dot(spread, up_z, preferred_element_type=F32)

    def order_green():
        green_copy.wait()

        def one(g, carry):
            for j in range(chunks):
                for t in range(0, padded_x, 8):
                    tile = green_raw[g, j * kc:(j + 1) * kc, t:t + 8, :]
                    tile = jnp.swapaxes(tile, 0, 1)
                    for h in range(halves):
                        green[j * halves + h, g, t:t + 8] = tile[:, :, h * 128:(h + 1) * 128]
            return carry

        lax.fori_loop(0, 6, one, 0)

    def send_raw(step, c, field):
        raw_out[c] = field
        remote(raw_out.at[c], raw_in.at[c], ws_sem.at[step, c], wr_sem.at[step, c], twin).start()

    def forward_z(c, which, field):
        dims = (((1,), (1,)), ((), ()))
        res = three_pass((wz_h[here], wz_l[here]), split(field), dims)
        out_t[c, which] = res.reshape(chunks, group, 2, kc, cells_y)

    def send_block(step, c, which, j):
        slab = me if which == 0 else twin

        def send(k, carry):
            to = lax.rem(seat + k, group)
            remote(
                out_t.at[c, which, j, to], in_t.at[c, j, slab], ts_sem.at[step, c, j], tr_sem.at[step, c, j], base + to
            ).start()
            return carry

        lax.fori_loop(1, group, send, 0)
        in_t[c, j, slab] = out_t[c, which, j, seat]

    def drain(view, sem):
        pltpu.make_async_copy(view, view, sem).wait()

    def forward_yx(step, c, j):
        drain(in_t.at[c, j, pl.ds(0, n - 2)], tr_sem.at[step, c, j])
        parts = [in_t[c, j, :, part].reshape(cells_x * kc, cells_y) for part in range(2)]
        dims = (((1,), (0,)), ((), ()))
        res = three_pass(split(jnp.concatenate(parts, axis=1)), (wy_h[...], wy_l[...]), dims)
        for part in range(2):
            for h in range(halves):
                at = part * padded_y + h * 128
                lines[j * halves + h, part] = res[:, at:at + 128].reshape(cells_x, kc, 128)

        def columns(h, carry):
            i = j * halves + h
            line = [(lines[i, 0, x], lines[i, 1, x]) for x in range(cells_x)]
            for m, (re, im) in enumerate(fft(line, -1)):
                spec[i, 2 * c, 2 * m], spec[i, 2 * c + 1, 2 * m] = re, im
            line = [twiddle(lines[i, 0, x], lines[i, 1, x], x, padded_x, -1) for x in range(cells_x)]
            for m, (re, im) in enumerate(fft(line, -1)):
                spec[i, 2 * c, 2 * m + 1], spec[i, 2 * c + 1, 2 * m + 1] = re, im
            return carry

        lax.fori_loop(0, halves, columns, 0)

    def backward_xy(step, a, j):
        row = COMBOS[a]

        def columns(h, carry):
            i = j * halves + h

            def field(k):
                g = [green[i, r, k] for r in row]
                s = [spec[i, r, k] for r in range(6)]
                return g[0] * s[0] + g[1] * s[2] + g[2] * s[4], g[0] * s[1] + g[1] * s[3] + g[2] * s[5]

            even = fft([field(k) for k in range(0, padded_x, 2)], 1)
            for x in range(cells_x):
                lines[i, 0, x], lines[i, 1, x] = even[x]
            odd = fft([field(k) for k in range(1, padded_x, 2)], 1)
            for x in range(cells_x):
                re, im = twiddle(*odd[x], x, padded_x, 1)
                lines[i, 0, x] += re
                lines[i, 1, x] += im
            return carry

        lax.fori_loop(0, halves, columns, 0)
        parts = [
            lines[j * halves + h, part].reshape(cells_x * kc, 128) for part in range(2) for h in range(halves)
        ]
        dims = (((1,), (0,)), ((), ()))
        res = three_pass(split(jnp.concatenate(parts, axis=1)), (vy_h[...], vy_l[...]), dims)
        for part in range(2):
            piece = res[:, part * cells_y:(part + 1) * cells_y]
            out_u[a, j, :, part] = piece.reshape(cells_x, kc, cells_y)
        send_back(step, a, j, 1, (1 - here) * group, cs_sem, cr_sem)
        send_back(step, a, j, 0, base, os_sem, or_sem)

    def send_back(step, a, j, which, first, s_sem, r_sem):
        def send(k, carry):
            to = lax.rem(seat + k, group)
            remote(
                out_u.at[a, j, first + to], in_u.at[a, which, j, seat], s_sem.at[step, a, j], r_sem.at[step, a, j],
                base + to,
            ).start()
            return carry

        lax.fori_loop(1, group, send, 0)
        in_u[a, which, j, seat] = out_u[a, j, first + seat]

    def inverse_z(a, which):
        field = in_u[a, which].reshape(chunks * group * 2 * kc, cells_y)
        return three_pass(split(field), (vz_h[here], vz_l[here]), (((0,), (0,)), ((), ())))

    def send_part(step, a):
        for j in range(chunks):
            drain(in_u.at[a, 1, j, pl.ds(0, group - 1)], cr_sem.at[step, a, j])
        part_out[a] = inverse_z(a, 1)
        remote(part_out.at[a], part_in.at[a], ps_sem.at[step, a], pr_sem.at[step, a], twin).start()

    loads[1].wait()
    for step in range(MATVECS):
        source, image = (pol_ref, first_ref) if step == 0 else (first_ref, second_ref)
        if step == 0:
            pl.semaphore_wait(barrier, group)
            for c in range(3):
                send_raw(step, c, source[c, 0] * mask_ref[...])
            for load in loads[2:]:
                load.wait()
            for c in range(3):
                forward_z(c, 0, raw_out[c])
                send_block(step, c, 0, 0)
            for j in range(1, chunks):
                for c in range(3):
                    send_block(step, c, 0, j)
            order_green()
        for c in range(3):
            drain(raw_in.at[c], wr_sem.at[step, c])
            forward_z(c, 1, raw_in[c])
            send_block(step, c, 1, 0)
        for j in range(1, chunks):
            for c in range(3):
                send_block(step, c, 1, j)
        for j in range(chunks):
            for c in range(3):
                forward_yx(step, c, j)
            for a in range(3):
                backward_xy(step, a, j)
                if j == chunks - 1 and a > 0:
                    send_part(step, a - 1)
        send_part(step, 2)
        for c in range(3):
            drain(raw_out.at[c], ws_sem.at[step, c])
            for j in range(chunks):
                drain(in_t.at[c, j, pl.ds(0, n - 2)], ts_sem.at[step, c, j])
        for a in range(3):
            for j in range(chunks):
                drain(in_u.at[a, 0, j, pl.ds(0, group - 1)], or_sem.at[step, a, j])
            own = inverse_z(a, 0)
            masked = source[a, 0] * mask_ref[...]
            drain(part_in.at[a], pr_sem.at[step, a])
            image[a, 0] = inv_ref[0] * masked - mask_ref[...] * (own + part_in[a])
            if step + 1 < MATVECS:
                send_raw(step + 1, a, image[a, 0] * mask_ref[...])
                forward_z(a, 0, raw_out[a])
                for j in range(chunks):
                    send_block(step + 1, a, 0, j)
        for a in range(3):
            for j in range(chunks):
                drain(in_u.at[a, 1, j, pl.ds(0, group - 1)], cs_sem.at[step, a, j])
                drain(in_u.at[a, 0, j, pl.ds(0, group - 1)], os_sem.at[step, a, j])
            drain(part_out.at[a], ps_sem.at[step, a])


def deliver(first, second, first_out, second_out, out_sem):
    stores = [
        pltpu.make_async_copy(held, target, out_sem.at[i])
        for i, (held, target) in enumerate(((first, first_out), (second, second_out)))
    ]
    for store in stores:
        store.start()
    for store in stores:
        store.wait()


def per_device(n, polarization, inverse_polarizability, occupancy, green_fourier):
    _, _, cells_y, cells_z = polarization.shape
    _, kz_own, padded_x, padded_y = green_fourier.shape
    padded_z = 2 * cells_z
    cells_x = padded_x // 2
    kc = min(8, kz_own)
    chunks = kz_own // kc
    halves = padded_y // 128
    group = n // 2

    def by_block(table):
        table = table.reshape(2, 2, group, chunks, kc, cells_z)
        return table.transpose(1, 3, 2, 0, 4, 5).reshape(2, chunks * group * 2 * kc, cells_z)

    cos, sin = tables(padded_z, cells_z, padded_z)
    wz = split_table(by_block(np.stack([cos, -sin])))
    vz = split_table(by_block(np.stack([cos, -sin])) / (padded_x * padded_y * padded_z))
    cos, sin = tables(cells_y, padded_y, padded_y)
    wy = split_table(np.block([[cos, -sin], [sin, cos]]))
    cos, sin = tables(padded_y, cells_y, padded_y)
    vy = split_table(np.block([[cos, sin], [-sin, cos]]))
    constants = [jnp.asarray(table) for table in wz + wy + vy + vz]
    anywhere = pl.BlockSpec(memory_space=pl.ANY)
    vmem = pl.BlockSpec(memory_space=pltpu.VMEM)
    dma = pltpu.SemaphoreType.DMA
    images = pl.pallas_call(
        functools.partial(kernel, n, cells_x, padded_x, kz_own, kc),
        out_shape=(pltpu.VMEM(polarization.shape, F32),) * 2,
        in_specs=[anywhere] * 12,
        out_specs=(vmem, vmem),
        scratch_shapes=[
            pltpu.VMEM(polarization.shape, F32),
            pltpu.VMEM(inverse_polarizability.shape, F32),
            pltpu.VMEM(occupancy.shape, jnp.int32),
            *[pltpu.VMEM(table.shape, BF16) for table in constants],
            pltpu.VMEM(green_fourier.shape, F32),
            pltpu.VMEM((chunks * halves, 6, padded_x, kc, 128), F32),
            pltpu.VMEM((cells_y, cells_z), F32),
            pltpu.VMEM((3, cells_y, cells_z), F32),
            pltpu.VMEM((3, cells_y, cells_z), F32),
            pltpu.VMEM((3, 2, chunks, group, 2, kc, cells_y), F32),
            pltpu.VMEM((3, chunks, n, 2, kc, cells_y), F32),
            pltpu.VMEM((chunks * halves, 2, cells_x, kc, 128), F32),
            pltpu.VMEM((chunks * halves, 6, padded_x, kc, 128), F32),
            pltpu.VMEM((3, chunks, n, 2, kc, cells_y), F32),
            pltpu.VMEM((3, 2, chunks, group, 2, kc, cells_y), F32),
            pltpu.VMEM((3, cells_y, cells_z), F32),
            pltpu.VMEM((3, cells_y, cells_z), F32),
            dma,
            dma((11,)),
            *[dma((MATVECS, 3))] * 2,
            *[dma((MATVECS, 3, chunks))] * 6,
            *[dma((MATVECS, 3))] * 2,
        ],
        compiler_params=pltpu.CompilerParams(
            collective_id=0, has_side_effects=True, vmem_limit_bytes=60 * 1024 * 1024
        ),
    )(polarization, inverse_polarizability, occupancy, green_fourier, *constants)
    return pl.pallas_call(
        deliver,
        out_shape=(jax.ShapeDtypeStruct(polarization.shape, F32),) * 2,
        in_specs=[vmem] * 2,
        out_specs=(anywhere, anywhere),
        scratch_shapes=[dma((2,))],
    )(*[pltpu.with_memory_space_constraint(x, pltpu.VMEM) for x in images])


def solution(mesh):
    return jax.shard_map(
        functools.partial(per_device, mesh.shape["slab"]),
        mesh=mesh,
        in_specs=(
            P("comp", "slab", None, None),
            P("slab", None, None),
            P("slab", None, None),
            P(None, "slab", None, None),
        ),
        out_specs=(P("comp", "slab", None, None), P("comp", "slab", None, None)),
        check_vma=False,
    )
```

```python
import functools
import math

import jax
import jax.numpy as jnp
import numpy as np
from jax import lax
from jax.experimental import pallas as pl
from jax.experimental.pallas import tpu as pltpu
from jax.sharding import PartitionSpec as P

BLOCK = 8
MATVECS = 2
SPLIT = 1
F32 = jnp.float32
BF16 = jnp.bfloat16
COMBOS = ((0, 3, 4), (3, 1, 5), (4, 5, 2))


def tables(count_in, count_out, length):
    phase = np.arange(count_in)[:, None] * np.arange(count_out)[None, :] % length
    angle = phase * (2.0 * math.pi / length)
    return np.cos(angle), np.sin(angle)


def split_table(table):
    table = table.astype(np.float32)
    high = table.astype(jnp.bfloat16)
    low = (table - high.astype(np.float32)).astype(jnp.bfloat16)
    return high, low


def split(value):
    high = value.astype(BF16)
    return high, (value - high.astype(F32)).astype(BF16)


def twiddle(re, im, num, length, sign):
    num = num * sign % length
    if num == 0:
        return re, im
    if 4 * num == length:
        return -im, re
    if 2 * num == length:
        return -re, -im
    if 4 * num == 3 * length:
        return im, -re
    c = math.cos(2.0 * math.pi * num / length)
    s = math.sin(2.0 * math.pi * num / length)
    if (8 * num) % length == 0:
        a = abs(c)
        p, m = (re + im) * a, (re - im) * a
        return {1: (m, p), 3: (-p, m), 5: (-m, -p), 7: (p, -m)}[8 * num // length]
    return re * c - im * s, re * s + im * c


def fft(values, sign):
    n = len(values)
    if n == 1:
        return values
    even, odd = fft(values[0::2], sign), fft(values[1::2], sign)
    low, high = [], []
    for k in range(n // 2):
        (er, ei), (o_r, oi) = even[k], twiddle(*odd[k], k, n, sign)
        low.append((er + o_r, ei + oi))
        high.append((er - o_r, ei - oi))
    return low + high


def three_pass(pair, table_pair, dims):
    dot = functools.partial(lax.dot_general, dimension_numbers=dims, preferred_element_type=F32)
    (vh, vl), (th, tl) = pair, table_pair
    return dot(vh, th) + (dot(vl, th) + dot(vh, tl))


def kernel(
    n, cells_x, padded_x, kz_own, kx, kc,
    pol_hbm, inv_hbm, occ_hbm, green_ref, *refs,
):
    tables_hbm, refs = refs[:8], refs[8:]
    first_ref, second_ref, pol_ref, inv_ref, occ_ref, *refs = refs
    tables_vmem, refs = refs[:8], refs[8:]
    wz_h, wz_l, wy_h, wy_l, vy_h, vy_l, vz_h, vz_l = tables_vmem
    (
        green_raw, green, mask_ref, raw_out, raw_in, out_t, in_t, lines, spec, out_u, in_u, part_out, part_in,
        green_sem, load_sem, ws_sem, wr_sem, ts_sem, tr_sem, cs_sem, cr_sem, os_sem, or_sem, ps_sem, pr_sem,
    ) = refs
    me = lax.axis_index("slab")
    group = n // 2
    here = me // group
    seat = lax.rem(me, group)
    plane = n // 4

    def twin_of(device):
        return n - plane - device + 2 * lax.rem(device, plane)

    twin = twin_of(me)
    base = here * group
    chunks, sub = kz_own // kx, kx // kc
    cells_y, cells_z = mask_ref.shape
    padded_y = 2 * cells_y
    halves = padded_y // 128

    def signal(device):
        pl.semaphore_signal(barrier, inc=1, device_id={"slab": device}, device_id_type=pl.DeviceIdType.MESH)

    def remote(source, target, send_sem, recv_sem, device):
        return pltpu.make_async_remote_copy(
            src_ref=source, dst_ref=target, send_sem=send_sem, recv_sem=recv_sem,
            device_id={"slab": device}, device_id_type=pl.DeviceIdType.MESH,
        )

    barrier = pltpu.get_barrier_semaphore()
    signal(twin)

    def greet(k, carry):
        signal(base + lax.rem(seat + k, group))
        return carry

    lax.fori_loop(1, group, greet, 0)
    sources = (occ_hbm, pol_hbm, inv_hbm, *tables_hbm)
    targets = (occ_ref, pol_ref, inv_ref, *tables_vmem)
    loads = [
        pltpu.make_async_copy(source, target, load_sem.at[i]) for i, (source, target) in enumerate(zip(sources, targets))
    ]
    for load in loads:
        load.start()
    green_copy = pltpu.make_async_copy(green_ref, green_raw, green_sem)
    green_copy.start()
    loads[0].wait()

    blocks_y, blocks_z = occ_ref.shape[1:]
    up_y = lax.broadcasted_iota(jnp.int32, (cells_y, blocks_y), 0) // BLOCK
    up_y = (up_y == lax.broadcasted_iota(jnp.int32, (cells_y, blocks_y), 1)).astype(F32).astype(BF16)
    up_z = lax.broadcasted_iota(jnp.int32, (blocks_z, cells_z), 1) // BLOCK
    up_z = (up_z == lax.broadcasted_iota(jnp.int32, (blocks_z, cells_z), 0)).astype(F32).astype(BF16)
    flags = occ_ref[0].astype(F32).astype(BF16)
    spread = jnp.dot(up_y, flags, preferred_element_type=F32).astype(BF16)
    mask_ref[...] = jnp.dot(spread, up_z, preferred_element_type=F32)

    def order_green():
        green_copy.wait()

        def one(g, carry):
            for j in range(chunks * sub):
                for t in range(0, padded_x, 8):
                    tile = green_raw[g, j * kc:(j + 1) * kc, t:t + 8, :]
                    tile = jnp.swapaxes(tile, 0, 1)
                    for h in range(halves):
                        green[j * halves + h, g, t:t + 8] = tile[:, :, h * 128:(h + 1) * 128]
            return carry

        lax.fori_loop(0, 6, one, 0)

    def send_raw(step, c, field):
        raw_out[c] = field
        remote(raw_out.at[c], raw_in.at[c], ws_sem.at[step, c], wr_sem.at[step, c], twin).start()

    def forward_z(c, which, field):
        dims = (((1,), (1,)), ((), ()))
        res = three_pass((wz_h[here], wz_l[here]), split(field), dims)
        out_t[c, which] = res.reshape(chunks, group, 2, kx, cells_y)

    def send_block(step, c, which, j):
        slab = me if which == 0 else twin

        def send(k, carry):
            to = lax.rem(seat + k, group)
            remote(
                out_t.at[c, which, j, to], in_t.at[c, j, slab], ts_sem.at[step, c, j], tr_sem.at[step, c, j], base + to
            ).start()
            return carry

        lax.fori_loop(1, group, send, 0)
        in_t[c, j, slab] = out_t[c, which, j, seat]

    def drain(view, sem):
        pltpu.make_async_copy(view, view, sem).wait()

    def forward_yx(step, c, j):
        drain(in_t.at[c, j, pl.ds(0, n - 2)], tr_sem.at[step, c, j])
        parts = [in_t[c, j, :, part].reshape(cells_x * kx, cells_y) for part in range(2)]
        dims = (((1,), (0,)), ((), ()))
        res = three_pass(split(jnp.concatenate(parts, axis=1)), (wy_h[...], wy_l[...]), dims)
        for part in range(2):
            for h in range(halves):
                at = part * padded_y + h * 128
                piece = res[:, at:at + 128].reshape(cells_x, kx, 128)
                for p in range(sub):
                    lines[(j * sub + p) * halves + h, part] = piece[:, p * kc:(p + 1) * kc]

        def columns(h, carry):
            i = j * sub * halves + h
            line = [(lines[i, 0, x], lines[i, 1, x]) for x in range(cells_x)]
            for m, (re, im) in enumerate(fft(line, -1)):
                spec[i, 2 * c, 2 * m], spec[i, 2 * c + 1, 2 * m] = re, im
            line = [twiddle(lines[i, 0, x], lines[i, 1, x], x, padded_x, -1) for x in range(cells_x)]
            for m, (re, im) in enumerate(fft(line, -1)):
                spec[i, 2 * c, 2 * m + 1], spec[i, 2 * c + 1, 2 * m + 1] = re, im
            return carry

        lax.fori_loop(0, sub * halves, columns, 0)

    def backward_xy(step, a, j):
        row = COMBOS[a]

        def columns(h, carry):
            i = j * sub * halves + h

            def field(k):
                g = [green[i, r, k] for r in row]
                s = [spec[i, r, k] for r in range(6)]
                return g[0] * s[0] + g[1] * s[2] + g[2] * s[4], g[0] * s[1] + g[1] * s[3] + g[2] * s[5]

            even = fft([field(k) for k in range(0, padded_x, 2)], 1)
            for x in range(cells_x):
                lines[i, 0, x], lines[i, 1, x] = even[x]
            odd = fft([field(k) for k in range(1, padded_x, 2)], 1)
            for x in range(cells_x):
                re, im = twiddle(*odd[x], x, padded_x, 1)
                lines[i, 0, x] += re
                lines[i, 1, x] += im
            return carry

        lax.fori_loop(0, sub * halves, columns, 0)
        parts = []
        for part in range(2):
            for h in range(halves):
                pieces = [lines[(j * sub + p) * halves + h, part] for p in range(sub)]
                piece = pieces[0] if sub == 1 else jnp.concatenate(pieces, axis=1)
                parts.append(piece.reshape(cells_x * kx, 128))
        dims = (((1,), (0,)), ((), ()))
        res = three_pass(split(jnp.concatenate(parts, axis=1)), (vy_h[...], vy_l[...]), dims)
        for part in range(2):
            piece = res[:, part * cells_y:(part + 1) * cells_y]
            out_u[a, j, :, part] = piece.reshape(cells_x, kx, cells_y)
        send_back(step, a, j, 1, twin_of, cs_sem, cr_sem)
        send_back(step, a, j, 0, lambda device: device, os_sem, or_sem)

    def send_back(step, a, j, which, slab_of, s_sem, r_sem):
        def send(k, carry):
            to = lax.rem(seat + k, group)
            remote(
                out_u.at[a, j, slab_of(base + to)], in_u.at[a, which, j, seat], s_sem.at[step, a, j], r_sem.at[step, a, j],
                base + to,
            ).start()
            return carry

        lax.fori_loop(1, group, send, 0)
        in_u[a, which, j, seat] = out_u[a, j, slab_of(me)]

    def inverse_z(a, which):
        field = in_u[a, which].reshape(chunks * group * 2 * kx, cells_y)
        return three_pass(split(field), (vz_h[here], vz_l[here]), (((0,), (0,)), ((), ())))

    def send_part(step, a):
        for j in range(chunks):
            drain(in_u.at[a, 1, j, pl.ds(0, group - 1)], cr_sem.at[step, a, j])
        part_out[a] = inverse_z(a, 1)
        remote(part_out.at[a], part_in.at[a], ps_sem.at[step, a], pr_sem.at[step, a], twin).start()

    loads[1].wait()
    for step in range(MATVECS):
        source, image = (pol_ref, first_ref) if step == 0 else (first_ref, second_ref)
        if step == 0:
            pl.semaphore_wait(barrier, group)
            for c in range(3):
                send_raw(step, c, source[c, 0] * mask_ref[...])
            for load in loads[2:]:
                load.wait()
            for c in range(3):
                forward_z(c, 0, raw_out[c])
                send_block(step, c, 0, 0)
            for j in range(1, chunks):
                for c in range(3):
                    send_block(step, c, 0, j)
            order_green()
        for c in range(3):
            drain(raw_in.at[c], wr_sem.at[step, c])
            forward_z(c, 1, raw_in[c])
            send_block(step, c, 1, 0)
        for j in range(1, chunks):
            for c in range(3):
                send_block(step, c, 1, j)
        for j in range(chunks):
            for c in range(3):
                forward_yx(step, c, j)
            for a in range(3):
                backward_xy(step, a, j)
                if j == chunks - 1 and a > 0:
                    send_part(step, a - 1)
        send_part(step, 2)
        for c in range(3):
            drain(raw_out.at[c], ws_sem.at[step, c])
            for j in range(chunks):
                drain(in_t.at[c, j, pl.ds(0, n - 2)], ts_sem.at[step, c, j])
        for a in range(3):
            for j in range(chunks):
                drain(in_u.at[a, 0, j, pl.ds(0, group - 1)], or_sem.at[step, a, j])
            own = inverse_z(a, 0)
            masked = source[a, 0] * mask_ref[...]
            drain(part_in.at[a], pr_sem.at[step, a])
            image[a, 0] = inv_ref[0] * masked - mask_ref[...] * (own + part_in[a])
            if step + 1 < MATVECS:
                send_raw(step + 1, a, image[a, 0] * mask_ref[...])
                forward_z(a, 0, raw_out[a])
                for j in range(chunks):
                    send_block(step + 1, a, 0, j)
        for a in range(3):
            for j in range(chunks):
                drain(in_u.at[a, 1, j, pl.ds(0, group - 1)], cs_sem.at[step, a, j])
                drain(in_u.at[a, 0, j, pl.ds(0, group - 1)], os_sem.at[step, a, j])
            drain(part_out.at[a], ps_sem.at[step, a])


def deliver(first, second, first_out, second_out, out_sem):
    stores = [
        pltpu.make_async_copy(held, target, out_sem.at[i])
        for i, (held, target) in enumerate(((first, first_out), (second, second_out)))
    ]
    for store in stores:
        store.start()
    for store in stores:
        store.wait()


def per_device(n, polarization, inverse_polarizability, occupancy, green_fourier):
    _, _, cells_y, cells_z = polarization.shape
    _, kz_own, padded_x, padded_y = green_fourier.shape
    padded_z = 2 * cells_z
    cells_x = padded_x // 2
    kx = kz_own // SPLIT if kz_own % (8 * SPLIT) == 0 else kz_own
    kc = min(8, kx)
    chunks = kz_own // kx
    halves = padded_y // 128
    group = n // 2

    def by_block(table):
        table = table.reshape(2, 2, group, chunks, kx, cells_z)
        return table.transpose(1, 3, 2, 0, 4, 5).reshape(2, chunks * group * 2 * kx, cells_z)

    cos, sin = tables(padded_z, cells_z, padded_z)
    wz = split_table(by_block(np.stack([cos, -sin])))
    vz = split_table(by_block(np.stack([cos, -sin])) / (padded_x * padded_y * padded_z))
    cos, sin = tables(cells_y, padded_y, padded_y)
    wy = split_table(np.block([[cos, -sin], [sin, cos]]))
    cos, sin = tables(padded_y, cells_y, padded_y)
    vy = split_table(np.block([[cos, sin], [-sin, cos]]))
    constants = [jnp.asarray(table) for table in wz + wy + vy + vz]
    anywhere = pl.BlockSpec(memory_space=pl.ANY)
    vmem = pl.BlockSpec(memory_space=pltpu.VMEM)
    dma = pltpu.SemaphoreType.DMA
    images = pl.pallas_call(
        functools.partial(kernel, n, cells_x, padded_x, kz_own, kx, kc),
        out_shape=(pltpu.VMEM(polarization.shape, F32),) * 2,
        in_specs=[anywhere] * 12,
        out_specs=(vmem, vmem),
        scratch_shapes=[
            pltpu.VMEM(polarization.shape, F32),
            pltpu.VMEM(inverse_polarizability.shape, F32),
            pltpu.VMEM(occupancy.shape, jnp.int32),
            *[pltpu.VMEM(table.shape, BF16) for table in constants],
            pltpu.VMEM(green_fourier.shape, F32),
            pltpu.VMEM((kz_own // kc * halves, 6, padded_x, kc, 128), F32),
            pltpu.VMEM((cells_y, cells_z), F32),
            pltpu.VMEM((3, cells_y, cells_z), F32),
            pltpu.VMEM((3, cells_y, cells_z), F32),
            pltpu.VMEM((3, 2, chunks, group, 2, kx, cells_y), F32),
            pltpu.VMEM((3, chunks, n, 2, kx, cells_y), F32),
            pltpu.VMEM((kz_own // kc * halves, 2, cells_x, kc, 128), F32),
            pltpu.VMEM((kz_own // kc * halves, 6, padded_x, kc, 128), F32),
            pltpu.VMEM((3, chunks, n, 2, kx, cells_y), F32),
            pltpu.VMEM((3, 2, chunks, group, 2, kx, cells_y), F32),
            pltpu.VMEM((3, cells_y, cells_z), F32),
            pltpu.VMEM((3, cells_y, cells_z), F32),
            dma,
            dma((11,)),
            *[dma((MATVECS, 3))] * 2,
            *[dma((MATVECS, 3, chunks))] * 6,
            *[dma((MATVECS, 3))] * 2,
        ],
        compiler_params=pltpu.CompilerParams(
            collective_id=0, has_side_effects=True, vmem_limit_bytes=60 * 1024 * 1024
        ),
    )(polarization, inverse_polarizability, occupancy, green_fourier, *constants)
    return pl.pallas_call(
        deliver,
        out_shape=(jax.ShapeDtypeStruct(polarization.shape, F32),) * 2,
        in_specs=[vmem] * 2,
        out_specs=(anywhere, anywhere),
        scratch_shapes=[dma((2,))],
    )(*[pltpu.with_memory_space_constraint(x, pltpu.VMEM) for x in images])


def solution(mesh):
    return jax.shard_map(
        functools.partial(per_device, mesh.shape["slab"]),
        mesh=mesh,
        in_specs=(
            P("comp", "slab", None, None),
            P("slab", None, None),
            P("slab", None, None),
            P(None, "slab", None, None),
        ),
        out_specs=(P("comp", "slab", None, None), P("comp", "slab", None, None)),
        check_vma=False,
    )
```

```python
import functools
import math

import jax
import jax.numpy as jnp
import numpy as np
from jax import lax
from jax.experimental import pallas as pl
from jax.experimental.pallas import tpu as pltpu
from jax.sharding import PartitionSpec as P

BLOCK = 8
MATVECS = 2
SPLIT = 1
STAGGER_NS = 3000
F32 = jnp.float32
BF16 = jnp.bfloat16
COMBOS = ((0, 3, 4), (3, 1, 5), (4, 5, 2))


def tables(count_in, count_out, length):
    phase = np.arange(count_in)[:, None] * np.arange(count_out)[None, :] % length
    angle = phase * (2.0 * math.pi / length)
    return np.cos(angle), np.sin(angle)


def split_table(table):
    table = table.astype(np.float32)
    high = table.astype(jnp.bfloat16)
    low = (table - high.astype(np.float32)).astype(jnp.bfloat16)
    return high, low


def split(value):
    high = value.astype(BF16)
    return high, (value - high.astype(F32)).astype(BF16)


def twiddle(re, im, num, length, sign):
    num = num * sign % length
    if num == 0:
        return re, im
    if 4 * num == length:
        return -im, re
    if 2 * num == length:
        return -re, -im
    if 4 * num == 3 * length:
        return im, -re
    c = math.cos(2.0 * math.pi * num / length)
    s = math.sin(2.0 * math.pi * num / length)
    if (8 * num) % length == 0:
        a = abs(c)
        p, m = (re + im) * a, (re - im) * a
        return {1: (m, p), 3: (-p, m), 5: (-m, -p), 7: (p, -m)}[8 * num // length]
    return re * c - im * s, re * s + im * c


def fft(values, sign):
    n = len(values)
    if n == 1:
        return values
    even, odd = fft(values[0::2], sign), fft(values[1::2], sign)
    low, high = [], []
    for k in range(n // 2):
        (er, ei), (o_r, oi) = even[k], twiddle(*odd[k], k, n, sign)
        low.append((er + o_r, ei + oi))
        high.append((er - o_r, ei - oi))
    return low + high


def three_pass(pair, table_pair, dims):
    dot = functools.partial(lax.dot_general, dimension_numbers=dims, preferred_element_type=F32)
    (vh, vl), (th, tl) = pair, table_pair
    return dot(vh, th) + (dot(vl, th) + dot(vh, tl))


def kernel(
    n, cells_x, padded_x, kz_own, kx, kc,
    pol_hbm, inv_hbm, occ_hbm, green_ref, *refs,
):
    tables_hbm, refs = refs[:8], refs[8:]
    first_ref, second_ref, pol_ref, inv_ref, occ_ref, *refs = refs
    tables_vmem, refs = refs[:8], refs[8:]
    wz_h, wz_l, wy_h, wy_l, vy_h, vy_l, vz_h, vz_l = tables_vmem
    (
        green_raw, green, mask_ref, raw_out, raw_in, out_t, in_t, lines, spec, out_u, in_u, part_out, part_in,
        green_sem, load_sem, ws_sem, wr_sem, ts_sem, tr_sem, cs_sem, cr_sem, os_sem, or_sem, ps_sem, pr_sem,
    ) = refs
    me = lax.axis_index("slab")
    group = n // 2
    here = me // group
    seat = lax.rem(me, group)
    plane = n // 4

    def twin_of(device):
        return n - plane - device + 2 * lax.rem(device, plane)

    twin = twin_of(me)
    base = here * group
    chunks, sub = kz_own // kx, kx // kc
    cells_y, cells_z = mask_ref.shape
    padded_y = 2 * cells_y
    halves = padded_y // 128

    def signal(device):
        pl.semaphore_signal(barrier, inc=1, device_id={"slab": device}, device_id_type=pl.DeviceIdType.MESH)

    def remote(source, target, send_sem, recv_sem, device):
        return pltpu.make_async_remote_copy(
            src_ref=source, dst_ref=target, send_sem=send_sem, recv_sem=recv_sem,
            device_id={"slab": device}, device_id_type=pl.DeviceIdType.MESH,
        )

    barrier = pltpu.get_barrier_semaphore()
    signal(twin)

    def greet(k, carry):
        signal(base + lax.rem(seat + k, group))
        return carry

    lax.fori_loop(1, group, greet, 0)
    sources = (occ_hbm, pol_hbm, inv_hbm, *tables_hbm)
    targets = (occ_ref, pol_ref, inv_ref, *tables_vmem)
    loads = [
        pltpu.make_async_copy(source, target, load_sem.at[i]) for i, (source, target) in enumerate(zip(sources, targets))
    ]
    for load in loads:
        load.start()
    green_copy = pltpu.make_async_copy(green_ref, green_raw, green_sem)
    green_copy.start()
    loads[0].wait()

    blocks_y, blocks_z = occ_ref.shape[1:]
    up_y = lax.broadcasted_iota(jnp.int32, (cells_y, blocks_y), 0) // BLOCK
    up_y = (up_y == lax.broadcasted_iota(jnp.int32, (cells_y, blocks_y), 1)).astype(F32).astype(BF16)
    up_z = lax.broadcasted_iota(jnp.int32, (blocks_z, cells_z), 1) // BLOCK
    up_z = (up_z == lax.broadcasted_iota(jnp.int32, (blocks_z, cells_z), 0)).astype(F32).astype(BF16)
    flags = occ_ref[0].astype(F32).astype(BF16)
    spread = jnp.dot(up_y, flags, preferred_element_type=F32).astype(BF16)
    mask_ref[...] = jnp.dot(spread, up_z, preferred_element_type=F32)

    def order_green():
        green_copy.wait()

        def one(g, carry):
            for j in range(chunks * sub):
                for t in range(0, padded_x, 8):
                    tile = green_raw[g, j * kc:(j + 1) * kc, t:t + 8, :]
                    tile = jnp.swapaxes(tile, 0, 1)
                    for h in range(halves):
                        green[j * halves + h, g, t:t + 8] = tile[:, :, h * 128:(h + 1) * 128]
            return carry

        lax.fori_loop(0, 6, one, 0)

    def send_raw(step, c, field):
        raw_out[c] = field
        remote(raw_out.at[c], raw_in.at[c], ws_sem.at[step, c], wr_sem.at[step, c], twin).start()

    def forward_z(c, which, field):
        dims = (((1,), (1,)), ((), ()))
        res = three_pass((wz_h[here], wz_l[here]), split(field), dims)
        out_t[c, which] = res.reshape(chunks, group, 2, kx, cells_y)

    def send_block(step, c, which, j):
        slab = me if which == 0 else twin

        def send(k, carry):
            to = lax.rem(seat + k, group)
            remote(
                out_t.at[c, which, j, to], in_t.at[c, j, slab], ts_sem.at[step, c, j], tr_sem.at[step, c, j], base + to
            ).start()
            return carry

        lax.fori_loop(1, group, send, 0)
        in_t[c, j, slab] = out_t[c, which, j, seat]

    def drain(view, sem):
        pltpu.make_async_copy(view, view, sem).wait()

    def forward_yx(step, c, j):
        drain(in_t.at[c, j, pl.ds(0, n - 2)], tr_sem.at[step, c, j])
        parts = [in_t[c, j, :, part].reshape(cells_x * kx, cells_y) for part in range(2)]
        dims = (((1,), (0,)), ((), ()))
        res = three_pass(split(jnp.concatenate(parts, axis=1)), (wy_h[...], wy_l[...]), dims)
        for part in range(2):
            for h in range(halves):
                at = part * padded_y + h * 128
                piece = res[:, at:at + 128].reshape(cells_x, kx, 128)
                for p in range(sub):
                    lines[(j * sub + p) * halves + h, part] = piece[:, p * kc:(p + 1) * kc]

        def columns(h, carry):
            i = j * sub * halves + h
            line = [(lines[i, 0, x], lines[i, 1, x]) for x in range(cells_x)]
            for m, (re, im) in enumerate(fft(line, -1)):
                spec[i, 2 * c, 2 * m], spec[i, 2 * c + 1, 2 * m] = re, im
            line = [twiddle(lines[i, 0, x], lines[i, 1, x], x, padded_x, -1) for x in range(cells_x)]
            for m, (re, im) in enumerate(fft(line, -1)):
                spec[i, 2 * c, 2 * m + 1], spec[i, 2 * c + 1, 2 * m + 1] = re, im
            return carry

        lax.fori_loop(0, sub * halves, columns, 0)

    def backward_xy(step, a, j):
        row = COMBOS[a]

        def columns(h, carry):
            i = j * sub * halves + h

            def field(k):
                g = [green[i, r, k] for r in row]
                s = [spec[i, r, k] for r in range(6)]
                return g[0] * s[0] + g[1] * s[2] + g[2] * s[4], g[0] * s[1] + g[1] * s[3] + g[2] * s[5]

            even = fft([field(k) for k in range(0, padded_x, 2)], 1)
            for x in range(cells_x):
                lines[i, 0, x], lines[i, 1, x] = even[x]
            odd = fft([field(k) for k in range(1, padded_x, 2)], 1)
            for x in range(cells_x):
                re, im = twiddle(*odd[x], x, padded_x, 1)
                lines[i, 0, x] += re
                lines[i, 1, x] += im
            return carry

        lax.fori_loop(0, sub * halves, columns, 0)
        parts = []
        for part in range(2):
            for h in range(halves):
                pieces = [lines[(j * sub + p) * halves + h, part] for p in range(sub)]
                piece = pieces[0] if sub == 1 else jnp.concatenate(pieces, axis=1)
                parts.append(piece.reshape(cells_x * kx, 128))
        dims = (((1,), (0,)), ((), ()))
        res = three_pass(split(jnp.concatenate(parts, axis=1)), (vy_h[...], vy_l[...]), dims)
        for part in range(2):
            piece = res[:, part * cells_y:(part + 1) * cells_y]
            out_u[a, j, :, part] = piece.reshape(cells_x, kx, cells_y)
        send_back(step, a, j, 1, twin_of, cs_sem, cr_sem)

    def send_back(step, a, j, which, slab_of, s_sem, r_sem):
        def send(k, carry):
            to = lax.rem(seat + k, group)
            remote(
                out_u.at[a, j, slab_of(base + to)], in_u.at[a, which, j, seat], s_sem.at[step, a, j], r_sem.at[step, a, j],
                base + to,
            ).start()
            return carry

        lax.fori_loop(1, group, send, 0)
        in_u[a, which, j, seat] = out_u[a, j, slab_of(me)]

    def send_home(step, a):
        for j in range(chunks):
            send_back(step, a, j, 0, lambda device: device, os_sem, or_sem)

    def inverse_z(a, which):
        field = in_u[a, which].reshape(chunks * group * 2 * kx, cells_y)
        return three_pass(split(field), (vz_h[here], vz_l[here]), (((0,), (0,)), ((), ())))

    def send_part(step, a):
        for j in range(chunks):
            drain(in_u.at[a, 1, j, pl.ds(0, group - 1)], cr_sem.at[step, a, j])
        part_out[a] = inverse_z(a, 1)
        remote(part_out.at[a], part_in.at[a], ps_sem.at[step, a], pr_sem.at[step, a], twin).start()

    loads[1].wait()
    for step in range(MATVECS):
        source, image = (pol_ref, first_ref) if step == 0 else (first_ref, second_ref)
        if step == 0:
            pl.semaphore_wait(barrier, group)
            pl.delay((1 - lax.axis_index("comp")) * STAGGER_NS)
            for c in range(3):
                send_raw(step, c, source[c, 0] * mask_ref[...])
            for load in loads[2:]:
                load.wait()
            for c in range(3):
                forward_z(c, 0, raw_out[c])
                send_block(step, c, 0, 0)
            for j in range(1, chunks):
                for c in range(3):
                    send_block(step, c, 0, j)
            order_green()
        for c in range(3):
            drain(raw_in.at[c], wr_sem.at[step, c])
            forward_z(c, 1, raw_in[c])
            send_block(step, c, 1, 0)
        for j in range(1, chunks):
            for c in range(3):
                send_block(step, c, 1, j)
        for j in range(chunks):
            for c in range(3):
                forward_yx(step, c, j)
            for a in range(3):
                backward_xy(step, a, j)
                if j == chunks - 1 and a > 0:
                    send_home(step, a - 1)
        for a in range(3):
            send_part(step, a)
            if a == 0:
                send_home(step, 2)
        for c in range(3):
            drain(raw_out.at[c], ws_sem.at[step, c])
            for j in range(chunks):
                drain(in_t.at[c, j, pl.ds(0, n - 2)], ts_sem.at[step, c, j])
        for a in range(3):
            for j in range(chunks):
                drain(in_u.at[a, 0, j, pl.ds(0, group - 1)], or_sem.at[step, a, j])
            own = inverse_z(a, 0)
            masked = source[a, 0] * mask_ref[...]
            drain(part_in.at[a], pr_sem.at[step, a])
            image[a, 0] = inv_ref[0] * masked - mask_ref[...] * (own + part_in[a])
            if step + 1 < MATVECS:
                send_raw(step + 1, a, image[a, 0] * mask_ref[...])
                forward_z(a, 0, raw_out[a])
                for j in range(chunks):
                    send_block(step + 1, a, 0, j)
        for a in range(3):
            for j in range(chunks):
                drain(in_u.at[a, 1, j, pl.ds(0, group - 1)], cs_sem.at[step, a, j])
                drain(in_u.at[a, 0, j, pl.ds(0, group - 1)], os_sem.at[step, a, j])
            drain(part_out.at[a], ps_sem.at[step, a])


def deliver(first, second, first_out, second_out, out_sem):
    stores = [
        pltpu.make_async_copy(held, target, out_sem.at[i])
        for i, (held, target) in enumerate(((first, first_out), (second, second_out)))
    ]
    for store in stores:
        store.start()
    for store in stores:
        store.wait()


def per_device(n, polarization, inverse_polarizability, occupancy, green_fourier):
    _, _, cells_y, cells_z = polarization.shape
    _, kz_own, padded_x, padded_y = green_fourier.shape
    padded_z = 2 * cells_z
    cells_x = padded_x // 2
    kx = kz_own // SPLIT if kz_own % (8 * SPLIT) == 0 else kz_own
    kc = min(8, kx)
    chunks = kz_own // kx
    halves = padded_y // 128
    group = n // 2

    def by_block(table):
        table = table.reshape(2, 2, group, chunks, kx, cells_z)
        return table.transpose(1, 3, 2, 0, 4, 5).reshape(2, chunks * group * 2 * kx, cells_z)

    cos, sin = tables(padded_z, cells_z, padded_z)
    wz = split_table(by_block(np.stack([cos, -sin])))
    vz = split_table(by_block(np.stack([cos, -sin])) / (padded_x * padded_y * padded_z))
    cos, sin = tables(cells_y, padded_y, padded_y)
    wy = split_table(np.block([[cos, -sin], [sin, cos]]))
    cos, sin = tables(padded_y, cells_y, padded_y)
    vy = split_table(np.block([[cos, sin], [-sin, cos]]))
    constants = [jnp.asarray(table) for table in wz + wy + vy + vz]
    anywhere = pl.BlockSpec(memory_space=pl.ANY)
    vmem = pl.BlockSpec(memory_space=pltpu.VMEM)
    dma = pltpu.SemaphoreType.DMA
    images = pl.pallas_call(
        functools.partial(kernel, n, cells_x, padded_x, kz_own, kx, kc),
        out_shape=(pltpu.VMEM(polarization.shape, F32),) * 2,
        in_specs=[anywhere] * 12,
        out_specs=(vmem, vmem),
        scratch_shapes=[
            pltpu.VMEM(polarization.shape, F32),
            pltpu.VMEM(inverse_polarizability.shape, F32),
            pltpu.VMEM(occupancy.shape, jnp.int32),
            *[pltpu.VMEM(table.shape, BF16) for table in constants],
            pltpu.VMEM(green_fourier.shape, F32),
            pltpu.VMEM((kz_own // kc * halves, 6, padded_x, kc, 128), F32),
            pltpu.VMEM((cells_y, cells_z), F32),
            pltpu.VMEM((3, cells_y, cells_z), F32),
            pltpu.VMEM((3, cells_y, cells_z), F32),
            pltpu.VMEM((3, 2, chunks, group, 2, kx, cells_y), F32),
            pltpu.VMEM((3, chunks, n, 2, kx, cells_y), F32),
            pltpu.VMEM((kz_own // kc * halves, 2, cells_x, kc, 128), F32),
            pltpu.VMEM((kz_own // kc * halves, 6, padded_x, kc, 128), F32),
            pltpu.VMEM((3, chunks, n, 2, kx, cells_y), F32),
            pltpu.VMEM((3, 2, chunks, group, 2, kx, cells_y), F32),
            pltpu.VMEM((3, cells_y, cells_z), F32),
            pltpu.VMEM((3, cells_y, cells_z), F32),
            dma,
            dma((11,)),
            *[dma((MATVECS, 3))] * 2,
            *[dma((MATVECS, 3, chunks))] * 6,
            *[dma((MATVECS, 3))] * 2,
        ],
        compiler_params=pltpu.CompilerParams(
            collective_id=0, has_side_effects=True, vmem_limit_bytes=60 * 1024 * 1024
        ),
    )(polarization, inverse_polarizability, occupancy, green_fourier, *constants)
    return pl.pallas_call(
        deliver,
        out_shape=(jax.ShapeDtypeStruct(polarization.shape, F32),) * 2,
        in_specs=[vmem] * 2,
        out_specs=(anywhere, anywhere),
        scratch_shapes=[dma((2,))],
    )(*[pltpu.with_memory_space_constraint(x, pltpu.VMEM) for x in images])


def solution(mesh):
    return jax.shard_map(
        functools.partial(per_device, mesh.shape["slab"]),
        mesh=mesh,
        in_specs=(
            P("comp", "slab", None, None),
            P("slab", None, None),
            P("slab", None, None),
            P(None, "slab", None, None),
        ),
        out_specs=(P("comp", "slab", None, None), P("comp", "slab", None, None)),
        check_vma=False,
    )
```

```python
import functools
import math

import jax
import jax.numpy as jnp
import numpy as np
from jax import lax
from jax.experimental import pallas as pl
from jax.experimental.pallas import tpu as pltpu
from jax.sharding import PartitionSpec as P

BLOCK = 8
MATVECS = 2
SPLIT = 1
STAGGER_NS = 3000
F32 = jnp.float32
BF16 = jnp.bfloat16
COMBOS = ((0, 3, 4), (3, 1, 5), (4, 5, 2))


def tables(count_in, count_out, length):
    phase = np.arange(count_in)[:, None] * np.arange(count_out)[None, :] % length
    angle = phase * (2.0 * math.pi / length)
    return np.cos(angle), np.sin(angle)


def split_table(table):
    table = table.astype(np.float32)
    high = table.astype(jnp.bfloat16)
    low = (table - high.astype(np.float32)).astype(jnp.bfloat16)
    return high, low


def split(value):
    high = value.astype(BF16)
    return high, (value - high.astype(F32)).astype(BF16)


def twiddle(re, im, num, length, sign):
    num = num * sign % length
    if num == 0:
        return re, im
    if 4 * num == length:
        return -im, re
    if 2 * num == length:
        return -re, -im
    if 4 * num == 3 * length:
        return im, -re
    c = math.cos(2.0 * math.pi * num / length)
    s = math.sin(2.0 * math.pi * num / length)
    if (8 * num) % length == 0:
        a = abs(c)
        p, m = (re + im) * a, (re - im) * a
        return {1: (m, p), 3: (-p, m), 5: (-m, -p), 7: (p, -m)}[8 * num // length]
    return re * c - im * s, re * s + im * c


def fft(values, sign):
    n = len(values)
    if n == 1:
        return values
    even, odd = fft(values[0::2], sign), fft(values[1::2], sign)
    low, high = [], []
    for k in range(n // 2):
        (er, ei), (o_r, oi) = even[k], twiddle(*odd[k], k, n, sign)
        low.append((er + o_r, ei + oi))
        high.append((er - o_r, ei - oi))
    return low + high


def three_pass(pair, table_pair, dims):
    dot = functools.partial(lax.dot_general, dimension_numbers=dims, preferred_element_type=F32)
    (vh, vl), (th, tl) = pair, table_pair
    return dot(vh, th) + (dot(vl, th) + dot(vh, tl))


def kernel(
    n, cells_x, padded_x, kz_own, kx, kc,
    pol_hbm, inv_hbm, occ_hbm, green_ref, *refs,
):
    tables_hbm, refs = refs[:8], refs[8:]
    first_ref, second_ref, pol_ref, inv_ref, occ_ref, *refs = refs
    tables_vmem, refs = refs[:8], refs[8:]
    wz_h, wz_l, wy_h, wy_l, vy_h, vy_l, vz_h, vz_l = tables_vmem
    (
        green_raw, green, mask_ref, raw_out, raw_in, out_t, in_t, lines, spec, out_u, in_u, part_out, part_in,
        green_sem, load_sem, ws_sem, wr_sem, ts_sem, tr_sem, cs_sem, cr_sem, os_sem, or_sem, ps_sem, pr_sem,
    ) = refs
    me = lax.axis_index("slab")
    group = n // 2
    here = me // group
    seat = lax.rem(me, group)
    plane = n // 4

    def twin_of(device):
        return n - plane - device + 2 * lax.rem(device, plane)

    twin = twin_of(me)
    base = here * group
    chunks, sub = kz_own // kx, kx // kc
    cells_y, cells_z = mask_ref.shape
    padded_y = 2 * cells_y
    halves = padded_y // 128

    def signal(device):
        pl.semaphore_signal(barrier, inc=1, device_id={"slab": device}, device_id_type=pl.DeviceIdType.MESH)

    def remote(source, target, send_sem, recv_sem, device):
        return pltpu.make_async_remote_copy(
            src_ref=source, dst_ref=target, send_sem=send_sem, recv_sem=recv_sem,
            device_id={"slab": device}, device_id_type=pl.DeviceIdType.MESH,
        )

    barrier = pltpu.get_barrier_semaphore()
    signal(twin)

    def greet(k, carry):
        signal(base + lax.rem(seat + k, group))
        return carry

    lax.fori_loop(1, group, greet, 0)
    sources = (occ_hbm, pol_hbm, inv_hbm, *tables_hbm)
    targets = (occ_ref, pol_ref, inv_ref, *tables_vmem)
    loads = [
        pltpu.make_async_copy(source, target, load_sem.at[i]) for i, (source, target) in enumerate(zip(sources, targets))
    ]
    for load in loads:
        load.start()
    green_copy = pltpu.make_async_copy(green_ref, green_raw, green_sem)
    green_copy.start()
    loads[0].wait()

    blocks_y, blocks_z = occ_ref.shape[1:]
    up_y = lax.broadcasted_iota(jnp.int32, (cells_y, blocks_y), 0) // BLOCK
    up_y = (up_y == lax.broadcasted_iota(jnp.int32, (cells_y, blocks_y), 1)).astype(F32).astype(BF16)
    up_z = lax.broadcasted_iota(jnp.int32, (blocks_z, cells_z), 1) // BLOCK
    up_z = (up_z == lax.broadcasted_iota(jnp.int32, (blocks_z, cells_z), 0)).astype(F32).astype(BF16)
    flags = occ_ref[0].astype(F32).astype(BF16)
    spread = jnp.dot(up_y, flags, preferred_element_type=F32).astype(BF16)
    mask_ref[...] = jnp.dot(spread, up_z, preferred_element_type=F32)

    def order_green():
        green_copy.wait()

        def one(g, carry):
            for j in range(chunks * sub):
                for t in range(0, padded_x, 8):
                    tile = green_raw[g, j * kc:(j + 1) * kc, t:t + 8, :]
                    tile = jnp.swapaxes(tile, 0, 1)
                    for h in range(halves):
                        green[j * halves + h, g, t:t + 8] = tile[:, :, h * 128:(h + 1) * 128]
            return carry

        lax.fori_loop(0, 6, one, 0)

    def send_raw(step, c, field):
        raw_out[c] = field
        remote(raw_out.at[c], raw_in.at[c], ws_sem.at[step, c], wr_sem.at[step, c], twin).start()

    def forward_z(c, which, field):
        dims = (((1,), (1,)), ((), ()))
        res = three_pass((wz_h[here], wz_l[here]), split(field), dims)
        out_t[c, which] = res.reshape(chunks, group, 2, kx, cells_y)

    def send_block(step, c, which, j):
        slab = me if which == 0 else twin

        def send(k, carry):
            to = seat ^ (group - k)
            remote(
                out_t.at[c, which, j, to], in_t.at[c, j, slab], ts_sem.at[step, c, j], tr_sem.at[step, c, j], base + to
            ).start()
            return carry

        lax.fori_loop(1, group, send, 0)
        in_t[c, j, slab] = out_t[c, which, j, seat]

    def drain(view, sem):
        pltpu.make_async_copy(view, view, sem).wait()

    def forward_yx(step, c, j):
        drain(in_t.at[c, j, pl.ds(0, n - 2)], tr_sem.at[step, c, j])
        parts = [in_t[c, j, :, part].reshape(cells_x * kx, cells_y) for part in range(2)]
        dims = (((1,), (0,)), ((), ()))
        res = three_pass(split(jnp.concatenate(parts, axis=1)), (wy_h[...], wy_l[...]), dims)
        for part in range(2):
            for h in range(halves):
                at = part * padded_y + h * 128
                piece = res[:, at:at + 128].reshape(cells_x, kx, 128)
                for p in range(sub):
                    lines[(j * sub + p) * halves + h, part] = piece[:, p * kc:(p + 1) * kc]

        def columns(h, carry):
            i = j * sub * halves + h
            line = [(lines[i, 0, x], lines[i, 1, x]) for x in range(cells_x)]
            for m, (re, im) in enumerate(fft(line, -1)):
                spec[i, 2 * c, 2 * m], spec[i, 2 * c + 1, 2 * m] = re, im
            line = [twiddle(lines[i, 0, x], lines[i, 1, x], x, padded_x, -1) for x in range(cells_x)]
            for m, (re, im) in enumerate(fft(line, -1)):
                spec[i, 2 * c, 2 * m + 1], spec[i, 2 * c + 1, 2 * m + 1] = re, im
            return carry

        lax.fori_loop(0, sub * halves, columns, 0)

    def backward_xy(step, a, j):
        row = COMBOS[a]

        def columns(h, carry):
            i = j * sub * halves + h

            def field(k):
                g = [green[i, r, k] for r in row]
                s = [spec[i, r, k] for r in range(6)]
                return g[0] * s[0] + g[1] * s[2] + g[2] * s[4], g[0] * s[1] + g[1] * s[3] + g[2] * s[5]

            even = fft([field(k) for k in range(0, padded_x, 2)], 1)
            for x in range(cells_x):
                lines[i, 0, x], lines[i, 1, x] = even[x]
            odd = fft([field(k) for k in range(1, padded_x, 2)], 1)
            for x in range(cells_x):
                re, im = twiddle(*odd[x], x, padded_x, 1)
                lines[i, 0, x] += re
                lines[i, 1, x] += im
            return carry

        lax.fori_loop(0, sub * halves, columns, 0)
        parts = []
        for part in range(2):
            for h in range(halves):
                pieces = [lines[(j * sub + p) * halves + h, part] for p in range(sub)]
                piece = pieces[0] if sub == 1 else jnp.concatenate(pieces, axis=1)
                parts.append(piece.reshape(cells_x * kx, 128))
        dims = (((1,), (0,)), ((), ()))
        res = three_pass(split(jnp.concatenate(parts, axis=1)), (vy_h[...], vy_l[...]), dims)
        for part in range(2):
            piece = res[:, part * cells_y:(part + 1) * cells_y]
            out_u[a, j, :, part] = piece.reshape(cells_x, kx, cells_y)
        send_back(step, a, j, 1, twin_of, cs_sem, cr_sem)

    def send_back(step, a, j, which, slab_of, s_sem, r_sem):
        def send(k, carry):
            to = seat ^ (group - k)
            remote(
                out_u.at[a, j, slab_of(base + to)], in_u.at[a, which, j, seat], s_sem.at[step, a, j], r_sem.at[step, a, j],
                base + to,
            ).start()
            return carry

        lax.fori_loop(1, group, send, 0)
        in_u[a, which, j, seat] = out_u[a, j, slab_of(me)]

    def send_home(step, a):
        for j in range(chunks):
            send_back(step, a, j, 0, lambda device: device, os_sem, or_sem)

    def inverse_z(a, which):
        field = in_u[a, which].reshape(chunks * group * 2 * kx, cells_y)
        return three_pass(split(field), (vz_h[here], vz_l[here]), (((0,), (0,)), ((), ())))

    def send_part(step, a):
        for j in range(chunks):
            drain(in_u.at[a, 1, j, pl.ds(0, group - 1)], cr_sem.at[step, a, j])
        part_out[a] = inverse_z(a, 1)
        remote(part_out.at[a], part_in.at[a], ps_sem.at[step, a], pr_sem.at[step, a], twin).start()

    loads[1].wait()
    for step in range(MATVECS):
        source, image = (pol_ref, first_ref) if step == 0 else (first_ref, second_ref)
        if step == 0:
            pl.semaphore_wait(barrier, group)
            pl.delay((1 - lax.axis_index("comp")) * STAGGER_NS)
            for c in range(3):
                send_raw(step, c, source[c, 0] * mask_ref[...])
            for load in loads[2:]:
                load.wait()
            for c in range(3):
                forward_z(c, 0, raw_out[c])
                send_block(step, c, 0, 0)
            for j in range(1, chunks):
                for c in range(3):
                    send_block(step, c, 0, j)
            order_green()
        for c in range(3):
            drain(raw_in.at[c], wr_sem.at[step, c])
            forward_z(c, 1, raw_in[c])
            send_block(step, c, 1, 0)
        for j in range(1, chunks):
            for c in range(3):
                send_block(step, c, 1, j)
        for j in range(chunks):
            for c in range(3):
                forward_yx(step, c, j)
            for a in range(3):
                backward_xy(step, a, j)
                if j == chunks - 1 and a > 0:
                    send_home(step, a - 1)
        for a in range(3):
            send_part(step, a)
            if a == 0:
                send_home(step, 2)
        for c in range(3):
            drain(raw_out.at[c], ws_sem.at[step, c])
            for j in range(chunks):
                drain(in_t.at[c, j, pl.ds(0, n - 2)], ts_sem.at[step, c, j])
        for a in range(3):
            for j in range(chunks):
                drain(in_u.at[a, 0, j, pl.ds(0, group - 1)], or_sem.at[step, a, j])
            own = inverse_z(a, 0)
            masked = source[a, 0] * mask_ref[...]
            drain(part_in.at[a], pr_sem.at[step, a])
            image[a, 0] = inv_ref[0] * masked - mask_ref[...] * (own + part_in[a])
            if step + 1 < MATVECS:
                send_raw(step + 1, a, image[a, 0] * mask_ref[...])
                forward_z(a, 0, raw_out[a])
                for j in range(chunks):
                    send_block(step + 1, a, 0, j)
        for a in range(3):
            for j in range(chunks):
                drain(in_u.at[a, 1, j, pl.ds(0, group - 1)], cs_sem.at[step, a, j])
                drain(in_u.at[a, 0, j, pl.ds(0, group - 1)], os_sem.at[step, a, j])
            drain(part_out.at[a], ps_sem.at[step, a])


def deliver(first, second, first_out, second_out, out_sem):
    stores = [
        pltpu.make_async_copy(held, target, out_sem.at[i])
        for i, (held, target) in enumerate(((first, first_out), (second, second_out)))
    ]
    for store in stores:
        store.start()
    for store in stores:
        store.wait()


def per_device(n, polarization, inverse_polarizability, occupancy, green_fourier):
    _, _, cells_y, cells_z = polarization.shape
    _, kz_own, padded_x, padded_y = green_fourier.shape
    padded_z = 2 * cells_z
    cells_x = padded_x // 2
    kx = kz_own // SPLIT if kz_own % (8 * SPLIT) == 0 else kz_own
    kc = min(8, kx)
    chunks = kz_own // kx
    halves = padded_y // 128
    group = n // 2

    def by_block(table):
        table = table.reshape(2, 2, group, chunks, kx, cells_z)
        return table.transpose(1, 3, 2, 0, 4, 5).reshape(2, chunks * group * 2 * kx, cells_z)

    cos, sin = tables(padded_z, cells_z, padded_z)
    wz = split_table(by_block(np.stack([cos, -sin])))
    vz = split_table(by_block(np.stack([cos, -sin])) / (padded_x * padded_y * padded_z))
    cos, sin = tables(cells_y, padded_y, padded_y)
    wy = split_table(np.block([[cos, -sin], [sin, cos]]))
    cos, sin = tables(padded_y, cells_y, padded_y)
    vy = split_table(np.block([[cos, sin], [-sin, cos]]))
    constants = [jnp.asarray(table) for table in wz + wy + vy + vz]
    anywhere = pl.BlockSpec(memory_space=pl.ANY)
    vmem = pl.BlockSpec(memory_space=pltpu.VMEM)
    dma = pltpu.SemaphoreType.DMA
    images = pl.pallas_call(
        functools.partial(kernel, n, cells_x, padded_x, kz_own, kx, kc),
        out_shape=(pltpu.VMEM(polarization.shape, F32),) * 2,
        in_specs=[anywhere] * 12,
        out_specs=(vmem, vmem),
        scratch_shapes=[
            pltpu.VMEM(polarization.shape, F32),
            pltpu.VMEM(inverse_polarizability.shape, F32),
            pltpu.VMEM(occupancy.shape, jnp.int32),
            *[pltpu.VMEM(table.shape, BF16) for table in constants],
            pltpu.VMEM(green_fourier.shape, F32),
            pltpu.VMEM((kz_own // kc * halves, 6, padded_x, kc, 128), F32),
            pltpu.VMEM((cells_y, cells_z), F32),
            pltpu.VMEM((3, cells_y, cells_z), F32),
            pltpu.VMEM((3, cells_y, cells_z), F32),
            pltpu.VMEM((3, 2, chunks, group, 2, kx, cells_y), F32),
            pltpu.VMEM((3, chunks, n, 2, kx, cells_y), F32),
            pltpu.VMEM((kz_own // kc * halves, 2, cells_x, kc, 128), F32),
            pltpu.VMEM((kz_own // kc * halves, 6, padded_x, kc, 128), F32),
            pltpu.VMEM((3, chunks, n, 2, kx, cells_y), F32),
            pltpu.VMEM((3, 2, chunks, group, 2, kx, cells_y), F32),
            pltpu.VMEM((3, cells_y, cells_z), F32),
            pltpu.VMEM((3, cells_y, cells_z), F32),
            dma,
            dma((11,)),
            *[dma((MATVECS, 3))] * 2,
            *[dma((MATVECS, 3, chunks))] * 6,
            *[dma((MATVECS, 3))] * 2,
        ],
        compiler_params=pltpu.CompilerParams(
            collective_id=0, has_side_effects=True, vmem_limit_bytes=60 * 1024 * 1024
        ),
    )(polarization, inverse_polarizability, occupancy, green_fourier, *constants)
    return pl.pallas_call(
        deliver,
        out_shape=(jax.ShapeDtypeStruct(polarization.shape, F32),) * 2,
        in_specs=[vmem] * 2,
        out_specs=(anywhere, anywhere),
        scratch_shapes=[dma((2,))],
    )(*[pltpu.with_memory_space_constraint(x, pltpu.VMEM) for x in images])


def solution(mesh):
    return jax.shard_map(
        functools.partial(per_device, mesh.shape["slab"]),
        mesh=mesh,
        in_specs=(
            P("comp", "slab", None, None),
            P("slab", None, None),
            P("slab", None, None),
            P(None, "slab", None, None),
        ),
        out_specs=(P("comp", "slab", None, None), P("comp", "slab", None, None)),
        check_vma=False,
    )
```

```python
import functools
import math

import jax
import jax.numpy as jnp
import numpy as np
from jax import lax
from jax.experimental import pallas as pl
from jax.experimental.pallas import tpu as pltpu
from jax.sharding import PartitionSpec as P

BLOCK = 8
MATVECS = 2
SPLIT = 1
STAGGER_NS = 3500
F32 = jnp.float32
BF16 = jnp.bfloat16
COMBOS = ((0, 3, 4), (3, 1, 5), (4, 5, 2))


def tables(count_in, count_out, length):
    phase = np.arange(count_in)[:, None] * np.arange(count_out)[None, :] % length
    angle = phase * (2.0 * math.pi / length)
    return np.cos(angle), np.sin(angle)


def split_table(table):
    table = table.astype(np.float32)
    high = table.astype(jnp.bfloat16)
    low = (table - high.astype(np.float32)).astype(jnp.bfloat16)
    return high, low


def split(value):
    high = value.astype(BF16)
    return high, (value - high.astype(F32)).astype(BF16)


def twiddle(re, im, num, length, sign):
    num = num * sign % length
    if num == 0:
        return re, im
    if 4 * num == length:
        return -im, re
    if 2 * num == length:
        return -re, -im
    if 4 * num == 3 * length:
        return im, -re
    c = math.cos(2.0 * math.pi * num / length)
    s = math.sin(2.0 * math.pi * num / length)
    if (8 * num) % length == 0:
        a = abs(c)
        p, m = (re + im) * a, (re - im) * a
        return {1: (m, p), 3: (-p, m), 5: (-m, -p), 7: (p, -m)}[8 * num // length]
    return re * c - im * s, re * s + im * c


def fft(values, sign):
    n = len(values)
    if n == 1:
        return values
    even, odd = fft(values[0::2], sign), fft(values[1::2], sign)
    low, high = [], []
    for k in range(n // 2):
        (er, ei), (o_r, oi) = even[k], twiddle(*odd[k], k, n, sign)
        low.append((er + o_r, ei + oi))
        high.append((er - o_r, ei - oi))
    return low + high


def three_pass(pair, table_pair, dims):
    dot = functools.partial(lax.dot_general, dimension_numbers=dims, preferred_element_type=F32)
    (vh, vl), (th, tl) = pair, table_pair
    return dot(vh, th) + (dot(vl, th) + dot(vh, tl))


def kernel(
    n, cells_x, padded_x, kz_own, kx, kc,
    pol_hbm, inv_hbm, occ_hbm, green_ref, *refs,
):
    tables_hbm, refs = refs[:8], refs[8:]
    first_ref, second_ref, pol_ref, inv_ref, occ_ref, *refs = refs
    tables_vmem, refs = refs[:8], refs[8:]
    wz_h, wz_l, wy_h, wy_l, vy_h, vy_l, vz_h, vz_l = tables_vmem
    (
        green_raw, green, mask_ref, raw_out, raw_in, out_t, in_t, lines, spec, out_u, in_u, part_out, part_in,
        green_sem, load_sem, ws_sem, wr_sem, ts_sem, tr_sem, cs_sem, cr_sem, os_sem, or_sem, ps_sem, pr_sem,
    ) = refs
    me = lax.axis_index("slab")
    group = n // 2
    here = me // group
    seat = lax.rem(me, group)
    plane = n // 4

    def twin_of(device):
        return n - plane - device + 2 * lax.rem(device, plane)

    twin = twin_of(me)
    base = here * group
    chunks, sub = kz_own // kx, kx // kc
    cells_y, cells_z = mask_ref.shape
    padded_y = 2 * cells_y
    halves = padded_y // 128

    def signal(device):
        pl.semaphore_signal(barrier, inc=1, device_id={"slab": device}, device_id_type=pl.DeviceIdType.MESH)

    def remote(source, target, send_sem, recv_sem, device):
        return pltpu.make_async_remote_copy(
            src_ref=source, dst_ref=target, send_sem=send_sem, recv_sem=recv_sem,
            device_id={"slab": device}, device_id_type=pl.DeviceIdType.MESH,
        )

    barrier = pltpu.get_barrier_semaphore()
    signal(twin)

    def greet(k, carry):
        signal(base + lax.rem(seat + k, group))
        return carry

    lax.fori_loop(1, group, greet, 0)
    sources = (occ_hbm, pol_hbm, inv_hbm, *tables_hbm)
    targets = (occ_ref, pol_ref, inv_ref, *tables_vmem)
    loads = [
        pltpu.make_async_copy(source, target, load_sem.at[i]) for i, (source, target) in enumerate(zip(sources, targets))
    ]
    for load in loads:
        load.start()
    green_copy = pltpu.make_async_copy(green_ref, green_raw, green_sem)
    green_copy.start()
    loads[0].wait()

    blocks_y, blocks_z = occ_ref.shape[1:]
    up_y = lax.broadcasted_iota(jnp.int32, (cells_y, blocks_y), 0) // BLOCK
    up_y = (up_y == lax.broadcasted_iota(jnp.int32, (cells_y, blocks_y), 1)).astype(F32).astype(BF16)
    up_z = lax.broadcasted_iota(jnp.int32, (blocks_z, cells_z), 1) // BLOCK
    up_z = (up_z == lax.broadcasted_iota(jnp.int32, (blocks_z, cells_z), 0)).astype(F32).astype(BF16)
    flags = occ_ref[0].astype(F32).astype(BF16)
    spread = jnp.dot(up_y, flags, preferred_element_type=F32).astype(BF16)
    mask_ref[...] = jnp.dot(spread, up_z, preferred_element_type=F32)

    def order_green():
        green_copy.wait()

        def one(g, carry):
            for j in range(chunks * sub):
                for t in range(0, padded_x, 8):
                    tile = green_raw[g, j * kc:(j + 1) * kc, t:t + 8, :]
                    tile = jnp.swapaxes(tile, 0, 1)
                    for h in range(halves):
                        green[j * halves + h, g, t:t + 8] = tile[:, :, h * 128:(h + 1) * 128]
            return carry

        lax.fori_loop(0, 6, one, 0)

    def send_raw(step, c, field):
        raw_out[c] = field
        remote(raw_out.at[c], raw_in.at[c], ws_sem.at[step, c], wr_sem.at[step, c], twin).start()

    def forward_z(c, which, field):
        dims = (((1,), (1,)), ((), ()))
        res = three_pass((wz_h[here], wz_l[here]), split(field), dims)
        out_t[c, which] = res.reshape(chunks, group, 2, kx, cells_y)

    def send_block(step, c, which, j):
        slab = me if which == 0 else twin

        def send(k, carry):
            to = seat ^ (group - k)
            remote(
                out_t.at[c, which, j, to], in_t.at[c, j, slab], ts_sem.at[step, c, j], tr_sem.at[step, c, j], base + to
            ).start()
            return carry

        lax.fori_loop(1, group, send, 0)
        in_t[c, j, slab] = out_t[c, which, j, seat]

    def drain(view, sem):
        pltpu.make_async_copy(view, view, sem).wait()

    def forward_yx(step, c, j):
        drain(in_t.at[c, j, pl.ds(0, n - 2)], tr_sem.at[step, c, j])
        parts = [in_t[c, j, :, part].reshape(cells_x * kx, cells_y) for part in range(2)]
        dims = (((1,), (0,)), ((), ()))
        res = three_pass(split(jnp.concatenate(parts, axis=1)), (wy_h[...], wy_l[...]), dims)
        for part in range(2):
            for h in range(halves):
                at = part * padded_y + h * 128
                piece = res[:, at:at + 128].reshape(cells_x, kx, 128)
                for p in range(sub):
                    lines[(j * sub + p) * halves + h, part] = piece[:, p * kc:(p + 1) * kc]

        def columns(h, carry):
            i = j * sub * halves + h
            line = [(lines[i, 0, x], lines[i, 1, x]) for x in range(cells_x)]
            for m, (re, im) in enumerate(fft(line, -1)):
                spec[i, 2 * c, 2 * m], spec[i, 2 * c + 1, 2 * m] = re, im
            line = [twiddle(lines[i, 0, x], lines[i, 1, x], x, padded_x, -1) for x in range(cells_x)]
            for m, (re, im) in enumerate(fft(line, -1)):
                spec[i, 2 * c, 2 * m + 1], spec[i, 2 * c + 1, 2 * m + 1] = re, im
            return carry

        lax.fori_loop(0, sub * halves, columns, 0)

    def backward_xy(step, a, j):
        row = COMBOS[a]

        def columns(h, carry):
            i = j * sub * halves + h

            def field(k):
                g = [green[i, r, k] for r in row]
                s = [spec[i, r, k] for r in range(6)]
                return g[0] * s[0] + g[1] * s[2] + g[2] * s[4], g[0] * s[1] + g[1] * s[3] + g[2] * s[5]

            even = fft([field(k) for k in range(0, padded_x, 2)], 1)
            for x in range(cells_x):
                lines[i, 0, x], lines[i, 1, x] = even[x]
            odd = fft([field(k) for k in range(1, padded_x, 2)], 1)
            for x in range(cells_x):
                re, im = twiddle(*odd[x], x, padded_x, 1)
                lines[i, 0, x] += re
                lines[i, 1, x] += im
            return carry

        lax.fori_loop(0, sub * halves, columns, 0)
        parts = []
        for part in range(2):
            for h in range(halves):
                pieces = [lines[(j * sub + p) * halves + h, part] for p in range(sub)]
                piece = pieces[0] if sub == 1 else jnp.concatenate(pieces, axis=1)
                parts.append(piece.reshape(cells_x * kx, 128))
        dims = (((1,), (0,)), ((), ()))
        res = three_pass(split(jnp.concatenate(parts, axis=1)), (vy_h[...], vy_l[...]), dims)
        for part in range(2):
            piece = res[:, part * cells_y:(part + 1) * cells_y]
            out_u[a, j, :, part] = piece.reshape(cells_x, kx, cells_y)
        send_back(step, a, j, 1, twin_of, cs_sem, cr_sem)

    def send_back(step, a, j, which, slab_of, s_sem, r_sem):
        def send(k, carry):
            to = seat ^ (group - k)
            remote(
                out_u.at[a, j, slab_of(base + to)], in_u.at[a, which, j, seat], s_sem.at[step, a, j], r_sem.at[step, a, j],
                base + to,
            ).start()
            return carry

        lax.fori_loop(1, group, send, 0)
        in_u[a, which, j, seat] = out_u[a, j, slab_of(me)]

    def send_home(step, a):
        for j in range(chunks):
            send_back(step, a, j, 0, lambda device: device, os_sem, or_sem)

    def inverse_z(a, which):
        field = in_u[a, which].reshape(chunks * group * 2 * kx, cells_y)
        return three_pass(split(field), (vz_h[here], vz_l[here]), (((0,), (0,)), ((), ())))

    def send_part(step, a):
        for j in range(chunks):
            drain(in_u.at[a, 1, j, pl.ds(0, group - 1)], cr_sem.at[step, a, j])
        part_out[a] = inverse_z(a, 1)
        remote(part_out.at[a], part_in.at[a], ps_sem.at[step, a], pr_sem.at[step, a], twin).start()

    loads[1].wait()
    for step in range(MATVECS):
        source, image = (pol_ref, first_ref) if step == 0 else (first_ref, second_ref)
        if step == 0:
            pl.semaphore_wait(barrier, group)
            pl.delay((1 - lax.axis_index("comp")) * STAGGER_NS)
            for c in range(3):
                send_raw(step, c, source[c, 0] * mask_ref[...])
            for load in loads[2:]:
                load.wait()
            for c in range(3):
                forward_z(c, 0, raw_out[c])
                send_block(step, c, 0, 0)
            for j in range(1, chunks):
                for c in range(3):
                    send_block(step, c, 0, j)
            order_green()
        for c in range(3):
            drain(raw_in.at[c], wr_sem.at[step, c])
            forward_z(c, 1, raw_in[c])
            send_block(step, c, 1, 0)
        for j in range(1, chunks):
            for c in range(3):
                send_block(step, c, 1, j)
        for j in range(chunks):
            for c in range(3):
                forward_yx(step, c, j)
            for a in range(3):
                backward_xy(step, a, j)
                if j == chunks - 1 and a > 0:
                    send_home(step, a - 1)
        for a in range(3):
            send_part(step, a)
            if a == 0:
                send_home(step, 2)
        for c in range(3):
            drain(raw_out.at[c], ws_sem.at[step, c])
            for j in range(chunks):
                drain(in_t.at[c, j, pl.ds(0, n - 2)], ts_sem.at[step, c, j])
        for a in range(3):
            for j in range(chunks):
                drain(in_u.at[a, 0, j, pl.ds(0, group - 1)], or_sem.at[step, a, j])
            own = inverse_z(a, 0)
            masked = source[a, 0] * mask_ref[...]
            drain(part_in.at[a], pr_sem.at[step, a])
            image[a, 0] = inv_ref[0] * masked - mask_ref[...] * (own + part_in[a])
            if step + 1 < MATVECS:
                send_raw(step + 1, a, image[a, 0] * mask_ref[...])
                forward_z(a, 0, raw_out[a])
                for j in range(chunks):
                    send_block(step + 1, a, 0, j)
        for a in range(3):
            for j in range(chunks):
                drain(in_u.at[a, 1, j, pl.ds(0, group - 1)], cs_sem.at[step, a, j])
                drain(in_u.at[a, 0, j, pl.ds(0, group - 1)], os_sem.at[step, a, j])
            drain(part_out.at[a], ps_sem.at[step, a])


def deliver(first, second, first_out, second_out, out_sem):
    stores = [
        pltpu.make_async_copy(held, target, out_sem.at[i])
        for i, (held, target) in enumerate(((first, first_out), (second, second_out)))
    ]
    for store in stores:
        store.start()
    for store in stores:
        store.wait()


def per_device(n, polarization, inverse_polarizability, occupancy, green_fourier):
    _, _, cells_y, cells_z = polarization.shape
    _, kz_own, padded_x, padded_y = green_fourier.shape
    padded_z = 2 * cells_z
    cells_x = padded_x // 2
    kx = kz_own // SPLIT if kz_own % (8 * SPLIT) == 0 else kz_own
    kc = min(8, kx)
    chunks = kz_own // kx
    halves = padded_y // 128
    group = n // 2

    def by_block(table):
        table = table.reshape(2, 2, group, chunks, kx, cells_z)
        return table.transpose(1, 3, 2, 0, 4, 5).reshape(2, chunks * group * 2 * kx, cells_z)

    cos, sin = tables(padded_z, cells_z, padded_z)
    wz = split_table(by_block(np.stack([cos, -sin])))
    vz = split_table(by_block(np.stack([cos, -sin])) / (padded_x * padded_y * padded_z))
    cos, sin = tables(cells_y, padded_y, padded_y)
    wy = split_table(np.block([[cos, -sin], [sin, cos]]))
    cos, sin = tables(padded_y, cells_y, padded_y)
    vy = split_table(np.block([[cos, sin], [-sin, cos]]))
    constants = [jnp.asarray(table) for table in wz + wy + vy + vz]
    anywhere = pl.BlockSpec(memory_space=pl.ANY)
    vmem = pl.BlockSpec(memory_space=pltpu.VMEM)
    dma = pltpu.SemaphoreType.DMA
    images = pl.pallas_call(
        functools.partial(kernel, n, cells_x, padded_x, kz_own, kx, kc),
        out_shape=(pltpu.VMEM(polarization.shape, F32),) * 2,
        in_specs=[anywhere] * 12,
        out_specs=(vmem, vmem),
        scratch_shapes=[
            pltpu.VMEM(polarization.shape, F32),
            pltpu.VMEM(inverse_polarizability.shape, F32),
            pltpu.VMEM(occupancy.shape, jnp.int32),
            *[pltpu.VMEM(table.shape, BF16) for table in constants],
            pltpu.VMEM(green_fourier.shape, F32),
            pltpu.VMEM((kz_own // kc * halves, 6, padded_x, kc, 128), F32),
            pltpu.VMEM((cells_y, cells_z), F32),
            pltpu.VMEM((3, cells_y, cells_z), F32),
            pltpu.VMEM((3, cells_y, cells_z), F32),
            pltpu.VMEM((3, 2, chunks, group, 2, kx, cells_y), F32),
            pltpu.VMEM((3, chunks, n, 2, kx, cells_y), F32),
            pltpu.VMEM((kz_own // kc * halves, 2, cells_x, kc, 128), F32),
            pltpu.VMEM((kz_own // kc * halves, 6, padded_x, kc, 128), F32),
            pltpu.VMEM((3, chunks, n, 2, kx, cells_y), F32),
            pltpu.VMEM((3, 2, chunks, group, 2, kx, cells_y), F32),
            pltpu.VMEM((3, cells_y, cells_z), F32),
            pltpu.VMEM((3, cells_y, cells_z), F32),
            dma,
            dma((11,)),
            *[dma((MATVECS, 3))] * 2,
            *[dma((MATVECS, 3, chunks))] * 6,
            *[dma((MATVECS, 3))] * 2,
        ],
        compiler_params=pltpu.CompilerParams(
            collective_id=0, has_side_effects=True, vmem_limit_bytes=60 * 1024 * 1024
        ),
    )(polarization, inverse_polarizability, occupancy, green_fourier, *constants)
    return pl.pallas_call(
        deliver,
        out_shape=(jax.ShapeDtypeStruct(polarization.shape, F32),) * 2,
        in_specs=[vmem] * 2,
        out_specs=(anywhere, anywhere),
        scratch_shapes=[dma((2,))],
    )(*[pltpu.with_memory_space_constraint(x, pltpu.VMEM) for x in images])


def solution(mesh):
    return jax.shard_map(
        functools.partial(per_device, mesh.shape["slab"]),
        mesh=mesh,
        in_specs=(
            P("comp", "slab", None, None),
            P("slab", None, None),
            P("slab", None, None),
            P(None, "slab", None, None),
        ),
        out_specs=(P("comp", "slab", None, None), P("comp", "slab", None, None)),
        check_vma=False,
    )
```
